32 devices in a mesh: seq: 16 (over z, y, core), head: 2 (over x).
Axes of the slice: x: 2, y: 2, z: 4, core: 2. Of those that a mesh axis runs over, the one named last changes fastest.
Arguments:
- q_main: bfloat16 [2048, 128, 576], P('seq', 'head'), may hold values from -6 to 6
- latent_keys: bfloat16 [2048, 576], P('seq'), may hold values from -6 to 6
- lse_main: float32 [2048, 128], P('seq', 'head'), may hold values from 0.5 to 2.5
- index_queries: bfloat16 [2048, 64, 128], P('seq', 'head'), may hold values from -6 to 6
- index_weights: float32 [2048, 64], P('seq', 'head'), may hold values from -1.5 to 1.5
- index_keys: bfloat16 [2048, 128], P('seq'), may hold values from -6 to 6
- lse_index: float32 [2048], P('seq'), may hold values from 0 to 2
- slab_order: int32 [16], replicated, may hold values from 0 to 15, each once
- block_live: int32 [16, 16], replicated, may hold values 0 or 1
Outputs:
- key_grad: float32 [2048, 128], P('seq')
The draws below stay inside these ranges and needn't reach their ends.
Inputs may be any that keep to these rules, and one draw needn't show every extreme that they name: `slab_order`: a permutation: every slab number once.
All inputs are finite; a program needn't handle non-finite values.
Results may differ from the reference program's by a relative error of at most 0.0028.
Values may be sent and summed in bfloat16 or wider, within the bound.
No kernel may reach another device: no remote copies, remote signals or barrier semaphores. Data moves between devices by JAX's collectives and lax.ppermute only.
A program may use at most 64 MiB of HBM per device.

```python
import jax
import jax.numpy as jnp
from jax import lax

HEADS = 128
LATENT = 576
IHEADS = 64
IDIM = 128
TOK_DEV = 128
HOPS = 8
TOKENS = 2048
N_SEQ = 16


def plant(array, rng, smallest, high):
    spot = [jax.random.randint(jax.random.fold_in(rng, axis), (), 0, length) for axis, length in enumerate(array.shape)]
    main_axis = array.shape.index(max(array.shape))
    neighbour = spot[:main_axis] + [(spot[main_axis] + 1) % array.shape[main_axis]] + spot[main_axis + 1:]
    return array.at[tuple(spot)].set(smallest).at[tuple(neighbour)].set(high)


def level_of(rng, extent, cuts, low, top_value):
    loudness, own = 1.0, jax.random.fold_in(rng, 6)
    for dim, parts in cuts:
        heights = jnp.exp(jax.random.uniform(jax.random.fold_in(own, dim), (parts,), jnp.float32, low / len(cuts), top_value / len(cuts)))
        loudness = loudness * jnp.repeat(heights, extent[dim] // parts).reshape([-1 if axis == dim else 1 for axis in range(len(extent))])
    return loudness


def noise(key, dims, spread, bound, cuts=(), held_as=jnp.bfloat16):
    entries = jax.random.normal(key, dims, jnp.float32) * spread
    if len(cuts) > 0:
        entries = level_of(key, dims, cuts, -0.22, 0.18) * entries
    return jnp.clip(entries, min=-bound, max=bound).astype(held_as)


def setup_inputs(seed: int = 0) -> dict:
    seeds = jax.random.split(jax.random.key(seed), 10)
    return {
        "q_main": noise(seeds[0], (TOKENS, HEADS, LATENT), 1.0, 6.0, ((0, 16), (1, 2))),
        "latent_keys": noise(seeds[1], (TOKENS, LATENT), 1.0, 6.0, ((0, 16),)),
        "lse_main": jnp.clip(0.5 + 2.0 * jax.random.uniform(seeds[2], (TOKENS, HEADS), jnp.float32) ** level_of(seeds[2], (TOKENS, HEADS), ((0, 16), (1, 2)), -0.2, 0.2), 0.5, 2.5),
        "index_queries": noise(seeds[3], (TOKENS, IHEADS, IDIM), 1.0, 6.0, ((0, 16), (1, 2))),
        "index_weights": noise(seeds[4], (TOKENS, IHEADS), 0.25, 1.5, ((0, 16), (1, 2)), jnp.float32),
        "index_keys": noise(seeds[5], (TOKENS, IDIM), 1.0, 6.0, ((0, 16),)),
        "lse_index": jnp.clip(2.0 * jax.random.uniform(seeds[6], (TOKENS,), jnp.float32) ** level_of(seeds[6], (TOKENS,), ((0, 16),), -0.2, 0.2), 0.0, 2.0),
        "slab_order": jax.random.permutation(seeds[7], N_SEQ).astype(jnp.int32),
        "block_live": plant((jax.random.randint(seeds[8], (N_SEQ, N_SEQ), 0, 4) < 3).astype(jnp.int32), jax.random.fold_in(seeds[8], 1), 0, 1),
    }


main_scale = 1.0 / 192.0 ** 0.5


def reference(q_main, latent_keys, lse_main, index_queries, index_weights, index_keys, lse_index, slab_order, block_live):
    index_scale = 1.0 / IDIM ** 0.5
    within = jnp.arange(TOK_DEV, dtype=jnp.int32)

    def one_block(key_place):
        key_slab = slab_order[key_place]
        key_start = (key_place * TOK_DEV).astype(jnp.int32)
        latent_block = lax.dynamic_slice_in_dim(latent_keys, key_start, TOK_DEV, 0).astype(jnp.float32)
        key_block = lax.dynamic_slice_in_dim(index_keys, key_start, TOK_DEV, 0).astype(jnp.float32)
        key_spots = key_slab * TOK_DEV + within
        key_total = jnp.zeros((TOK_DEV, IDIM), jnp.float32)
        for cycle_step in range(HOPS):
            query_place = ((key_place + cycle_step) % N_SEQ).astype(jnp.int32)
            query_slab = slab_order[query_place]
            query_start = (query_place * TOK_DEV).astype(jnp.int32)
            queries = lax.dynamic_slice_in_dim(q_main, query_start, TOK_DEV, 0).astype(jnp.float32)
            lse_rows = lax.dynamic_slice_in_dim(lse_main, query_start, TOK_DEV, 0)
            index_rows = lax.dynamic_slice_in_dim(index_queries, query_start, TOK_DEV, 0).astype(jnp.float32)
            weight_rows = lax.dynamic_slice_in_dim(index_weights, query_start, TOK_DEV, 0)
            lse_query = lax.dynamic_slice_in_dim(lse_index, query_start, TOK_DEV, 0)
            query_spots = query_slab * TOK_DEV + within
            scores = jnp.einsum("thc,kc->thk", queries, latent_block) * main_scale
            head_mass = jnp.sum(jnp.exp(scores - lse_rows[:, :, None]), axis=1)
            relu_input = jnp.einsum("tjc,kc->tjk", index_rows, key_block) * index_scale
            logits = jnp.sum(weight_rows[:, :, None] * jnp.maximum(relu_input, 0.0), axis=1)
            live_mask = (key_spots[None, :] <= query_spots[:, None]) & (block_live[query_slab, key_slab] == 1)
            grad_tile = jnp.where(live_mask, jnp.exp(logits - lse_query[:, None]) - head_mass / HEADS, 0.0)
            weighted = jnp.where(relu_input > 0.0, grad_tile[:, None, :] * weight_rows[:, :, None], 0.0).astype(jnp.bfloat16)
            summed = jnp.einsum("tjk,tjc->kc", weighted.astype(jnp.float32), index_rows)
            key_total = key_total + summed * index_scale
        return key_total

    blocks = lax.map(one_block, jnp.arange(N_SEQ, dtype=jnp.int32))
    return blocks.reshape(TOKENS, IDIM)
```

```python
import functools
import math

import jax
import jax.numpy as jnp
from jax import lax
from jax.experimental import pallas as pl
from jax.experimental.pallas import tpu as pltpu
from jax.sharding import PartitionSpec as P

HEADS = 128
HOPS = 8
LOG2E = math.log2(math.e)
MAIN_SCALE = 1.0 / 192.0**0.5
NT = (((1,), (1,)), ((), ()))
NN = (((1,), (0,)), ((), ()))


def score_kernel(idx_width, group, place_ref, q_ref, lse_ref, ka_ref, kb_ref, own_ref, away_ref, keys):
    step = pl.program_id(0)
    share = own_ref.shape[0] // q_ref.shape[0] if own_ref.shape[0] >= q_ref.shape[0] else 1
    rows = ka_ref.shape[0]
    tokens, heads, width = q_ref.shape

    @pl.when(step == 0)
    def _():
        keys[:rows] = ka_ref[:, idx_width:]
        keys[rows:] = kb_ref[:, idx_width:]

    held = keys[...]
    sums = []
    for first in range(0, tokens, group):
        q = q_ref[first : first + group].reshape(group * heads, width)
        s = lax.dot_general(q, held, NT, preferred_element_type=jnp.float32)
        s = s * (MAIN_SCALE * LOG2E)
        for t in range(group):
            part = s[t * heads : (t + 1) * heads]
            lse = lse_ref[0, :, first + t : first + t + 1]
            sums.append(jnp.sum(jnp.exp2(part - lse), axis=0, keepdims=True))
    tile = jnp.concatenate(sums, axis=0)

    @pl.when(step < share)
    def _():
        own_ref[pl.ds(pl.multiple_of(step * tokens, tokens), tokens), :] = tile

    @pl.when(step >= share)
    def _():
        away_ref[pl.ds(pl.multiple_of((step - share) * tokens, tokens), tokens), :] = tile


def head_mass(place, q_main, lse_steps, block_a, block_b, idx_width, n_head, tokens):
    total, heads, width = q_main.shape
    rows = block_a.shape[0]
    share = total // n_head
    steps = total // tokens
    per_share = share // tokens

    def turned(i, place_ref):
        return lax.rem(i + place_ref[0] * per_share, steps)

    whole = lambda shape: pl.BlockSpec(shape, lambda i, place_ref: (0,) * len(shape))
    return pl.pallas_call(
        functools.partial(score_kernel, idx_width, min(4, tokens)),
        grid_spec=pltpu.PrefetchScalarGridSpec(
            num_scalar_prefetch=1,
            grid=(steps,),
            in_specs=[
                pl.BlockSpec((tokens, heads, width), lambda i, p: (turned(i, p), 0, 0)),
                pl.BlockSpec((1, heads, tokens), lambda i, p: (turned(i, p), 0, 0)),
                whole(block_a.shape),
                whole(block_b.shape),
            ],
            out_specs=[whole((share, 2 * rows)), whole((total - share, 2 * rows))],
            scratch_shapes=[pltpu.VMEM((2 * rows, width), jnp.bfloat16)],
        ),
        out_shape=[
            jax.ShapeDtypeStruct((share, 2 * rows), jnp.float32),
            jax.ShapeDtypeStruct((total - share, 2 * rows), jnp.float32),
        ],
        cost_estimate=pl.CostEstimate(
            flops=2 * total * heads * width * 2 * rows * 2,
            transcendentals=total * heads * 2 * rows,
            bytes_accessed=total * heads * width * 2,
        ),
        name="score_mass",
    )(place, q_main, lse_steps, block_a, block_b)


def logit_kernel(idx_width, scale, lanes, *refs):
    *parts, w_ref, lse_ref, ka_ref, kb_ref, out_ref = refs
    share = lse_ref.shape[1]
    keys = jnp.concatenate([ka_ref[:, :idx_width], kb_ref[:, :idx_width]], axis=0)
    acc = jnp.zeros((keys.shape[0], lanes), jnp.float32)
    at = 0
    for part in parts:
        count = part.shape[0] * part.shape[1]
        flat = part[...].reshape(count, idx_width)
        for first in range(0, count, lanes):
            r = lax.dot_general(
                keys, flat[first : first + lanes], NT, preferred_element_type=jnp.float32
            )
            acc = acc + jnp.maximum(r * scale, 0.0) * w_ref[:, at : at + lanes]
            at += lanes
    logits = acc[:, :share]
    for first in range(share, lanes, share):
        logits = logits + acc[:, first : first + share]
    out_ref[...] = jnp.exp(logits - lse_ref[...])


def grad_kernel(idx_width, scale, lanes, n_mass, info_ref, *refs):
    n_parts = len(refs) - n_mass - 6
    parts, masses = refs[:n_parts], refs[n_parts : n_parts + n_mass]
    w_ref, target_ref, ka_ref, kb_ref, ga_ref, gb_ref = refs[n_parts + n_mass :]
    rows = ka_ref.shape[0]
    share = target_ref.shape[1]
    keys = jnp.concatenate([ka_ref[:, :idx_width], kb_ref[:, :idx_width]], axis=0)
    mass = masses[0][...]
    for other in masses[1:]:
        mass = mass + other[...]
    value = target_ref[...] - mass.T * (1.0 / HEADS)
    within = lax.broadcasted_iota(jnp.int32, (rows, share), 0)
    token = lax.broadcasted_iota(jnp.int32, (rows, share), 1) + info_ref[4]
    tiles = []
    for block in range(2):
        live = (within + info_ref[2 * block] <= token) & (info_ref[2 * block + 1] == 1)
        tiles.append(jnp.where(live, value[block * rows : (block + 1) * rows], 0.0))
    grad = jnp.concatenate(tiles, axis=0)
    grad = jnp.concatenate([grad] * (lanes // share), axis=1)
    total = jnp.zeros((2 * rows, idx_width), jnp.float32)
    at = 0
    for part in parts:
        count = part.shape[0] * part.shape[1]
        flat = part[...].reshape(count, idx_width)
        for first in range(0, count, lanes):
            piece = flat[first : first + lanes]
            r = lax.dot_general(keys, piece, NT, preferred_element_type=jnp.float32)
            weighted = jnp.where(r * scale > 0.0, grad * w_ref[:, at : at + lanes], 0.0)
            total = total + lax.dot_general(
                weighted.astype(jnp.bfloat16), piece, NN, preferred_element_type=jnp.float32
            )
            at += lanes
    ga_ref[...] = total[:rows] * scale
    gb_ref[...] = total[rows:] * scale


VMEM = pl.BlockSpec(memory_space=pltpu.VMEM)


def local(
    q_main,
    latent_keys,
    lse_main,
    index_queries,
    index_weights,
    index_keys,
    lse_index,
    slab_order,
    block_live,
):
    n_seq = lax.axis_size("seq")
    n_head = lax.axis_size("head")
    seq_place = lax.axis_index("seq")
    head_place = lax.axis_index("head")
    rows = latent_keys.shape[0]
    tokens_all, heads_here, _ = q_main.shape
    index_here = index_queries.shape[1]
    idx_width = index_keys.shape[1]
    scale = 1.0 / idx_width**0.5
    share = tokens_all // n_head
    devices = range(n_seq)

    odd = seq_place % 2
    forward = [(i, (i + (HOPS - 1 if i % 2 else 1)) % n_seq) for i in devices]
    back = [(b, a) for a, b in forward]
    swap = [(i, i ^ 1) for i in devices]

    def ring(distance):
        return [(i, (i + distance) % n_seq) for i in devices]

    own = jnp.concatenate([index_keys, latent_keys], axis=1)
    slots = [own, lax.ppermute(own, "seq", forward)]
    hops = [0 * odd, jnp.where(odd == 1, 1, HOPS - 1)]
    for m in range(1, HOPS // 2):
        got = lax.ppermute(own, "seq", ring(2 * m))
        slots += [got, lax.ppermute(got, "seq", swap)]
        hops += [0 * odd + 2 * m, jnp.where(odd == 1, 2 * m + 1, 2 * m - 1)]

    places = jnp.arange(n_seq, dtype=jnp.int32)
    own_slab = jnp.sum(jnp.where(places == seq_place, slab_order, 0))
    live_row = jnp.sum(jnp.where((places == own_slab)[:, None], block_live, 0), axis=0)
    sources = (seq_place - jnp.stack(hops)) % n_seq
    slabs = jnp.sum(jnp.where(places[None, :] == sources[:, None], slab_order[None, :], 0), axis=1)
    allowed = jnp.sum(jnp.where(places[None, :] == slabs[:, None], live_row[None, :], 0), axis=1)
    shift = (slabs - own_slab) * rows
    first_token = jnp.broadcast_to(head_place * share, (HOPS // 2, 1))
    info = jnp.concatenate([jnp.stack([shift, allowed], 1).reshape(HOPS // 2, 4), first_token], 1)
    info = info.astype(jnp.int32)

    turned_q = index_queries.transpose(1, 0, 2)
    turned_w = index_weights.T

    def to_share(array, axis, turn):
        start = lax.rem(head_place + turn, n_head) * share
        part = lax.dynamic_slice_in_dim(array, start, share, axis)
        if turn == 0:
            return part
        route = [(i, (i + turn) % n_head) for i in range(n_head)]
        return lax.ppermute(part, "head", route)

    parts = [to_share(turned_q, 1, turn) for turn in range(n_head)]
    weights = [to_share(turned_w, 1, turn).reshape(1, index_here * share) for turn in range(n_head)]
    w_flat = jnp.concatenate(weights, axis=1)
    lse_share = lax.dynamic_slice_in_dim(lse_index, head_place * share, share, 0)[None, :]
    lanes = min(256, index_here * share)

    tokens = min(16, share)
    lse_steps = (lse_main * LOG2E).reshape(tokens_all // tokens, tokens, heads_here)
    lse_steps = lse_steps.transpose(0, 2, 1)
    place = head_place.astype(jnp.int32)[None]

    masses = []
    for c in range(HOPS // 2):
        a, b = slots[2 * c], slots[2 * c + 1]
        near, away = head_mass(place, q_main, lse_steps, a, b, idx_width, n_head, tokens)
        got = [near]
        for turn in range(1, n_head):
            route = [(i, (i + turn) % n_head) for i in range(n_head)]
            part = away if n_head == 2 else away[(turn - 1) * share : turn * share]
            got.append(lax.ppermute(part, "head", route))
        masses.append(got)

    total = None
    for c in range(HOPS // 2):
        a, b = slots[2 * c], slots[2 * c + 1]
        target = pl.pallas_call(
            functools.partial(logit_kernel, idx_width, scale, lanes),
            in_specs=[VMEM] * (n_head + 4),
            out_specs=VMEM,
            out_shape=jax.ShapeDtypeStruct((2 * rows, share), jnp.float32),
            cost_estimate=pl.CostEstimate(
                flops=2 * 2 * rows * share * n_head * index_here * idx_width,
                transcendentals=2 * rows * share,
                bytes_accessed=2 * share * n_head * index_here * idx_width,
            ),
            name="index_logits",
        )(*parts, w_flat, lse_share, a, b)
        grad_a, grad_b = pl.pallas_call(
            functools.partial(grad_kernel, idx_width, scale, lanes, n_head),
            in_specs=[pl.BlockSpec(memory_space=pltpu.SMEM)] + [VMEM] * (2 * n_head + 4),
            out_specs=[VMEM, VMEM],
            out_shape=[jax.ShapeDtypeStruct((rows, idx_width), jnp.float32)] * 2,
            cost_estimate=pl.CostEstimate(
                flops=4 * 2 * rows * share * n_head * index_here * idx_width,
                transcendentals=0,
                bytes_accessed=2 * share * n_head * index_here * idx_width,
            ),
            name="index_grad",
        )(info[c], *parts, *masses[c], w_flat, target, a, b)
        if c == 0:
            total = grad_a + lax.ppermute(grad_b, "seq", back)
        else:
            both = grad_a + lax.ppermute(grad_b, "seq", swap)
            total = total + lax.ppermute(both, "seq", ring(-2 * c))
    if n_head == 2:
        return total + lax.ppermute(total, "head", [(0, 1), (1, 0)])
    return lax.psum(total, "head")


def solution(mesh):
    placed = (
        P("seq", "head", None),
        P("seq", None),
        P("seq", "head"),
        P("seq", "head", None),
        P("seq", "head"),
        P("seq", None),
        P("seq"),
        P(),
        P(),
    )
    return jax.shard_map(
        local, mesh=mesh, in_specs=placed, out_specs=P("seq", None), check_vma=False
    )
```

```python
import functools
import math

import jax
import jax.numpy as jnp
from jax import lax
from jax.experimental import pallas as pl
from jax.experimental.pallas import tpu as pltpu
from jax.sharding import PartitionSpec as P

HEADS = 128
HOPS = 8
LOG2E = math.log2(math.e)
MAIN_SCALE = 1.0 / 192.0**0.5
NT = (((1,), (1,)), ((), ()))
NN = (((1,), (0,)), ((), ()))
VMEM = pl.BlockSpec(memory_space=pltpu.VMEM)
SMEM = pl.BlockSpec(memory_space=pltpu.SMEM)


def score_kernel(latent, place_ref, q_ref, lse_ref, ka_ref, kb_ref, *outs):
    rows = ka_ref.shape[1]
    heads, _, tokens = q_ref.shape
    keys = jnp.concatenate([ka_ref[:latent, :].T, kb_ref[:latent, :].T], axis=0)
    total = None
    for h in range(0, heads, 2):
        pair = jnp.concatenate([q_ref[h], q_ref[h + 1]], axis=1)
        s = lax.dot_general(keys, pair, NN, preferred_element_type=jnp.float32)
        s = s * (MAIN_SCALE * LOG2E)
        for n in range(2):
            lse = lse_ref[h + n : h + n + 1, :] * LOG2E
            p = jnp.exp2(s[:, n * tokens : (n + 1) * tokens] - lse)
            total = p if total is None else total + p
    share = tokens // len(outs)
    turned = pltpu.roll(total, tokens - place_ref[0] * share, 1) if len(outs) > 1 else total
    for n, out in enumerate(outs):
        span = slice(n * share, (n + 1) * share)
        out[...] = jnp.concatenate([turned[:rows, span], turned[rows:, span]], axis=1)


def head_mass(place, q, lse, block_a, block_b, n_head):
    heads, latent, tokens = q.shape
    rows = block_a.shape[1]
    share = tokens // n_head
    return pl.pallas_call(
        functools.partial(score_kernel, latent),
        in_specs=[SMEM] + [VMEM] * 4,
        out_specs=[VMEM] * n_head,
        out_shape=[jax.ShapeDtypeStruct((rows, 2 * share), jnp.float32)] * n_head,
        cost_estimate=pl.CostEstimate(
            flops=2 * tokens * heads * latent * 2 * rows,
            transcendentals=tokens * heads * 2 * rows,
            bytes_accessed=tokens * heads * latent * 2,
        ),
        compiler_params=pltpu.CompilerParams(vmem_limit_bytes=LIMIT),
        name="score_mass",
    )(place, q, lse, block_a, block_b)


LIMIT = 16 * 2**20


def logit_kernel(latent, scale, lanes, *refs):
    *parts, w_ref, lse_ref, ka_ref, kb_ref, out_ref = refs
    share = lse_ref.shape[1]
    rows = ka_ref.shape[1]
    idx_width = parts[0].shape[2]
    fold = min(128, lanes)
    keys = jnp.concatenate([ka_ref[latent:, :], kb_ref[latent:, :]], axis=0)
    acc = jnp.zeros((2 * rows, fold), jnp.float32)
    at = 0
    for part in parts:
        count = part.shape[0] * part.shape[1]
        for first in range(0, count, lanes):
            piece = part[first // share : (first + lanes) // share].reshape(lanes, idx_width)
            r = lax.dot_general(keys, piece, NT, preferred_element_type=jnp.float32)
            for f in range(0, lanes, fold):
                acc = acc + jnp.maximum(r[:, f : f + fold], 0.0) * w_ref[:, at + f : at + f + fold]
            at += lanes
    logits = acc[:, :share]
    for first in range(share, fold, share):
        logits = logits + acc[:, first : first + share]
    value = jnp.exp(logits * scale - lse_ref[...])
    out_ref[...] = jnp.concatenate([value[:rows], value[rows:]], axis=1)


def grad_kernel(latent, scale, lanes, n_mass, info_ref, *refs):
    n_parts = len(refs) - n_mass - 6
    parts, masses = refs[:n_parts], refs[n_parts : n_parts + n_mass]
    w_ref, target_ref, ka_ref, kb_ref, ga_ref, gb_ref = refs[n_parts + n_mass :]
    rows = ka_ref.shape[1]
    share = target_ref.shape[1] // 2
    idx_width = ga_ref.shape[1]
    keys = jnp.concatenate([ka_ref[latent:, :], kb_ref[latent:, :]], axis=0)
    mass = masses[0][...]
    for other in masses[1:]:
        mass = mass + other[...]
    value = target_ref[...] - mass * (1.0 / HEADS)
    within = lax.broadcasted_iota(jnp.int32, (rows, share), 0)
    token = lax.broadcasted_iota(jnp.int32, (rows, share), 1) + info_ref[4]
    fold = min(128, lanes)
    tiles = []
    for block in range(2):
        live = (within + info_ref[2 * block] <= token) & (info_ref[2 * block + 1] == 1)
        tile = jnp.where(live, value[:, block * share : (block + 1) * share], 0.0)
        tiles.append(jnp.concatenate([tile] * (fold // share), axis=1))
    grad = jnp.concatenate(tiles, axis=0)
    total = jnp.zeros((2 * rows, idx_width), jnp.float32)
    at = 0
    for part in parts:
        count = part.shape[0] * part.shape[1]
        for first in range(0, count, lanes):
            piece = part[first // share : (first + lanes) // share].reshape(lanes, idx_width)
            r = lax.dot_general(keys, piece, NT, preferred_element_type=jnp.float32)
            ws = []
            for f in range(0, lanes, fold):
                ws.append(jnp.where(r[:, f : f + fold] > 0.0, grad * w_ref[:, at + f : at + f + fold], 0.0).astype(jnp.bfloat16))
            total = total + lax.dot_general(jnp.concatenate(ws, axis=1), piece, NN, preferred_element_type=jnp.float32)
            at += lanes
    ga_ref[...] = total[:rows] * scale
    gb_ref[...] = total[rows:] * scale


def index_logits(parts, w, lse, a, b, latent, lanes):
    n_head, (index_here, share, idx_width), rows = len(parts), parts[0].shape, a.shape[1]
    return pl.pallas_call(
        functools.partial(logit_kernel, latent, 1.0 / idx_width**0.5, lanes),
        in_specs=[VMEM] * (n_head + 4),
        out_specs=VMEM,
        out_shape=jax.ShapeDtypeStruct((rows, 2 * share), jnp.float32),
        cost_estimate=pl.CostEstimate(
            flops=2 * 2 * rows * share * n_head * index_here * idx_width,
            transcendentals=2 * rows * share,
            bytes_accessed=2 * share * n_head * index_here * idx_width,
        ),
        compiler_params=pltpu.CompilerParams(vmem_limit_bytes=LIMIT),
        name="index_logits",
    )(*parts, w, lse, a, b)


def index_grad(info, parts, masses, w, target, a, b, latent, lanes):
    n_head, (index_here, share, idx_width), rows = len(parts), parts[0].shape, a.shape[1]
    return pl.pallas_call(
        functools.partial(grad_kernel, latent, 1.0 / idx_width**0.5, lanes, len(masses)),
        in_specs=[SMEM] + [VMEM] * (n_head + len(masses) + 4),
        out_specs=[VMEM, VMEM],
        out_shape=[jax.ShapeDtypeStruct((rows, idx_width), jnp.float32)] * 2,
        cost_estimate=pl.CostEstimate(
            flops=4 * 2 * rows * share * n_head * index_here * idx_width,
            transcendentals=0,
            bytes_accessed=2 * share * n_head * index_here * idx_width,
        ),
        compiler_params=pltpu.CompilerParams(vmem_limit_bytes=LIMIT),
        name="index_grad",
    )(info, *parts, *masses, w, target, a, b)


def local(
    q_main,
    latent_keys,
    lse_main,
    index_queries,
    index_weights,
    index_keys,
    lse_index,
    slab_order,
    block_live,
):
    n_seq = lax.axis_size("seq")
    n_head = lax.axis_size("head")
    seq_place = lax.axis_index("seq")
    head_place = lax.axis_index("head")
    rows, latent = latent_keys.shape
    tokens_all = q_main.shape[0]
    index_here = index_queries.shape[1]
    share = tokens_all // n_head
    devices = range(n_seq)

    odd = seq_place % 2
    forward = [(i, (i + (HOPS - 1 if i % 2 else 1)) % n_seq) for i in devices]
    back = [(b, a) for a, b in forward]
    swap = [(i, i ^ 1) for i in devices]

    def ring(distance):
        return [(i, (i + distance) % n_seq) for i in devices]

    own = jnp.concatenate([latent_keys.T, index_keys], axis=0)
    two = lax.ppermute(own, "seq", ring(2))
    four = lax.ppermute(own, "seq", ring(4))
    slots = [own, lax.ppermute(own, "seq", forward)]
    hops = [0 * odd, jnp.where(odd == 1, 1, HOPS - 1)]
    arrived = [two, four]
    for m in range(1, HOPS // 2):
        if m > 2:
            arrived.append(lax.ppermute(arrived[m - 3], "seq", ring(4)))
        got = arrived[m - 1]
        slots += [got, lax.ppermute(got, "seq", swap)]
        hops += [0 * odd + 2 * m, jnp.where(odd == 1, 2 * m + 1, 2 * m - 1)]

    places = jnp.arange(n_seq, dtype=jnp.int32)
    own_slab = jnp.sum(jnp.where(places == seq_place, slab_order, 0))
    live_row = jnp.sum(jnp.where((places == own_slab)[:, None], block_live, 0), axis=0)
    sources = (seq_place - jnp.stack(hops)) % n_seq
    slabs = jnp.sum(jnp.where(places[None, :] == sources[:, None], slab_order[None, :], 0), axis=1)
    allowed = jnp.sum(jnp.where(places[None, :] == slabs[:, None], live_row[None, :], 0), axis=1)
    shift = (slabs - own_slab) * rows
    first_token = jnp.broadcast_to(head_place * share, (HOPS // 2, 1))
    info = jnp.concatenate([jnp.stack([shift, allowed], 1).reshape(HOPS // 2, 4), first_token], 1)
    info = info.astype(jnp.int32)

    def to_share(array, axis, turn):
        start = lax.rem(head_place + turn, n_head) * share
        part = lax.dynamic_slice_in_dim(array, start, share, axis)
        if turn == 0:
            return part
        route = [(i, (i + turn) % n_head) for i in range(n_head)]
        return lax.ppermute(part, "head", route)

    parts = [to_share(index_queries, 0, turn).transpose(1, 0, 2) for turn in range(n_head)]
    weights = [
        to_share(index_weights.T, 1, turn).reshape(1, index_here * share) for turn in range(n_head)
    ]
    w_flat = jnp.concatenate(weights, axis=1)
    lse_share = lax.dynamic_slice_in_dim(lse_index, head_place * share, share, 0)[None, :]
    lanes = min(1024, index_here * share)

    place = head_place.astype(jnp.int32)[None]
    turned_q = q_main.transpose(1, 2, 0)
    turned_lse = lse_main.T

    masses = []
    for c in range(HOPS // 2):
        a, b = slots[2 * c], slots[2 * c + 1]
        got = list(head_mass(place, turned_q, turned_lse, a, b, n_head))
        for turn in range(1, n_head):
            route = [(i, (i + turn) % n_head) for i in range(n_head)]
            got[turn] = lax.ppermute(got[turn], "head", route)
        masses.append(got)

    total = None
    for c in range(HOPS // 2):
        a, b = slots[2 * c], slots[2 * c + 1]
        target = index_logits(parts, w_flat, lse_share, a, b, latent, lanes)
        grad_a, grad_b = index_grad(info[c], parts, masses[c], w_flat, target, a, b, latent, lanes)
        if c == 0:
            total = grad_a + lax.ppermute(grad_b, "seq", back)
        else:
            both = grad_a + lax.ppermute(grad_b, "seq", swap)
            total = total + lax.ppermute(both, "seq", ring(-2 * c))
    if n_head == 2:
        return total + lax.ppermute(total, "head", [(0, 1), (1, 0)])
    return lax.psum(total, "head")


def solution(mesh):
    placed = (
        P("seq", "head", None),
        P("seq", None),
        P("seq", "head"),
        P("seq", "head", None),
        P("seq", "head"),
        P("seq", None),
        P("seq"),
        P(),
        P(),
    )
    return jax.shard_map(
        local, mesh=mesh, in_specs=placed, out_specs=P("seq", None), check_vma=False
    )
```

```python
import functools
import math

import jax
import jax.numpy as jnp
from jax import lax
from jax.experimental import pallas as pl
from jax.experimental.pallas import tpu as pltpu
from jax.sharding import PartitionSpec as P


HEADS = 128
HOPS = 8
LAST = 2
PIECES = 8
LOG2E = math.log2(math.e)
MAIN_SCALE = 1.0 / 192.0**0.5
LIMIT = 20 * 2**20
WHOLE = 49 * 2**20
NT = (((1,), (1,)), ((), ()))
NN = (((1,), (0,)), ((), ()))
VMEM = pl.BlockSpec(memory_space=pltpu.VMEM)
SMEM = pl.BlockSpec(memory_space=pltpu.SMEM)
HBM = pl.BlockSpec(memory_space=pltpu.HBM)


def facts(slot, order_ref, live_ref):
    n = lax.axis_size("seq")
    me = lax.axis_index("seq")
    crossed = (slot % 2 == 1) & (me % 2 == 0)
    hop = jnp.where(crossed, jnp.where(slot == 1, HOPS - 1, slot - 2), slot)
    own = order_ref[me]
    slab = order_ref[lax.rem(me - hop + n, n)]
    return slab - own, (slab <= own) & (live_ref[own, slab] == 1)


def mass_of(keys, q_ref, lse_ref, span):
    tokens = q_ref.shape[2]
    total = None
    for h in span[::2]:
        pair = jnp.concatenate([q_ref[h], q_ref[h + 1]], axis=1)
        s = lax.dot_general(keys, pair, NN, preferred_element_type=jnp.float32)
        s = s * (MAIN_SCALE * LOG2E)
        for n in range(2):
            lse = lse_ref[h + n : h + n + 1, :] * LOG2E
            p = jnp.exp2(s[:, n * tokens : (n + 1) * tokens] - lse)
            total = p if total is None else total + p
    return total


def cost(flops):
    return pl.CostEstimate(flops=flops, transcendentals=0, bytes_accessed=flops // 256)


def score_kernel(first, n_blocks, n_head, order_ref, live_ref, q_hbm, lse_ref, *refs):
    n_outs = n_head if n_blocks > 1 else 1
    blocks, known = refs[:n_blocks], refs[n_blocks : -n_outs - 4]
    outs, (q_ref, keys, mass, sems) = refs[-n_outs - 4 : -4], refs[-4:]
    heads, latent, tokens = q_ref.shape
    rows = blocks[0].shape[1]
    base = len(known)
    piece = max(2, heads // PIECES)
    spans = [range(h, h + piece) for h in range(0, heads, piece)]
    copies = []
    for i, span in enumerate(spans):
        part = pl.ds(span[0], piece)
        copies.append(pltpu.make_async_copy(q_hbm.at[part], q_ref.at[part], sems.at[i]))
        copies[i].start()
    for i in range(base):
        mass[i] = known[i][...]
    for i in range(n_blocks):
        keys[i] = blocks[i][:latent, :].T
    total = None
    for i, span in enumerate(spans):
        copies[i].wait()
        part = mass_of(keys[0], q_ref, lse_ref, span)
        total = part if total is None else total + part
    mass[base] = total

    def one_slot(i, carry):
        alive = facts(first + i, order_ref, live_ref)[1]

        @pl.when(alive)
        def _():
            mass[base + i] = mass_of(keys[i], q_ref, lse_ref, range(heads))

        @pl.when(jnp.logical_not(alive))
        def _():
            mass[base + i] = jnp.zeros((rows, tokens), jnp.float32)

        return carry

    if n_blocks == 1:
        outs[0][...] = total
        return
    lax.fori_loop(1, n_blocks, one_slot, 0)
    share = tokens // n_head
    turn = tokens - lax.axis_index("head") * share
    for c in range((base + n_blocks) // 2):
        pair = [pltpu.roll(mass[2 * c + n], turn, 1) if n_head > 1 else mass[2 * c + n] for n in range(2)]
        for n, out in enumerate(outs):
            span = slice(n * share, (n + 1) * share)
            out[c * rows : (c + 1) * rows, :] = jnp.concatenate([x[:, span] for x in pair], axis=1)


def head_mass(order, live, q, lse, blocks, known, first, n_head):
    heads, latent, tokens = q.shape
    rows = blocks[0].shape[1]
    share = tokens // n_head
    total = len(blocks) + len(known)
    shape = jax.ShapeDtypeStruct((total // 2 * rows, 2 * share), jnp.float32)
    shapes = [shape] * n_head
    if total == 1:
        shapes = [jax.ShapeDtypeStruct((rows, tokens), jnp.float32)]
    return pl.pallas_call(
        functools.partial(score_kernel, first, len(blocks), n_head),
        in_specs=[SMEM, SMEM, HBM] + [VMEM] * (1 + total),
        out_specs=[VMEM] * len(shapes),
        out_shape=shapes,
        scratch_shapes=[
            pltpu.VMEM(q.shape, q.dtype),
            pltpu.VMEM((len(blocks), rows, latent), jnp.bfloat16),
            pltpu.VMEM((total, rows, tokens), jnp.float32),
            pltpu.SemaphoreType.DMA((heads // max(2, heads // PIECES),)),
        ],
        cost_estimate=cost(2 * tokens * heads * latent * len(blocks) * rows),
        compiler_params=pltpu.CompilerParams(vmem_limit_bytes=WHOLE),
        name="score_mass",
    )(order, live, q, lse, *blocks, *known)


def lanes_of(part, share):
    return max(1, min(part.shape[0], 128 // share))


def pieces(part, share, width):
    side = lanes_of(part, share)
    step = part.shape[0] // side
    run = max(1, min(step, width))
    for first in range(0, step, run):
        heads = [part[k + n * step] for k in range(first, first + run) for n in range(side)]
        yield first, run, jnp.concatenate(heads, axis=0)


def lay_weights(parts, w_refs, w_lanes):
    at = 0
    for part, w_ref in zip(parts, w_refs):
        index_here, tokens = w_ref.shape
        share = part.shape[1]
        w = w_ref[...]
        if share < tokens:
            w = pltpu.roll(w, tokens - lax.axis_index("head") * share, 1)
        side = lanes_of(part, share)
        step = index_here // side
        tile = [w[n * step : (n + 1) * step, :share] for n in range(side)]
        w_lanes[at : at + step, :] = jnp.concatenate(tile, axis=1)
        at += step


def logit_kernel(latent, n_head, order_ref, live_ref, *refs):
    parts, w_refs, lse_ref = refs[:n_head], refs[n_head : 2 * n_head], refs[2 * n_head]
    blocks, (out_ref, w_ref, keys, values) = refs[2 * n_head + 1 : -4], refs[-4:]
    rows, idx_width = keys.shape[1:]
    share = parts[0].shape[1]
    scale = 1.0 / idx_width**0.5
    lay_weights(parts, w_refs, w_ref)
    tile = w_ref.shape[1]
    lse = lse_ref[...]
    if share < lse.shape[1]:
        lse = pltpu.roll(lse, lse.shape[1] - lax.axis_index("head") * share, 1)[:, :share]
    for i, block in enumerate(blocks):
        keys[i] = block[latent:, :]

    def one_slot(i, carry):
        @pl.when(facts(i, order_ref, live_ref)[1])
        def _():
            held = keys[i]
            acc = jnp.zeros((rows, tile), jnp.float32)
            at = 0
            for part in parts:
                for _, run, piece in pieces(part, share, 8):
                    r = lax.dot_general(held, piece, NT, preferred_element_type=jnp.float32)
                    for k in range(run):
                        relu = jnp.maximum(r[:, k * tile : (k + 1) * tile], 0.0)
                        acc = acc + relu * w_ref[at + k : at + k + 1, :]
                    at += run
            logits = acc[:, :share]
            for first in range(share, tile, share):
                logits = logits + acc[:, first : first + share]
            values[i] = jnp.exp(logits * scale - lse)

        return carry

    lax.fori_loop(0, len(blocks), one_slot, 0)
    for c in range(len(blocks) // 2):
        pair = [values[2 * c], values[2 * c + 1]]
        out_ref[c * rows : (c + 1) * rows, :] = jnp.concatenate(pair, axis=1)


def index_logits(order, live, parts, weights, lse, blocks, latent):
    n_head, (index_here, share, idx_width) = len(parts), parts[0].shape
    rows = blocks[0].shape[1]
    side = lanes_of(parts[0], share)
    return pl.pallas_call(
        functools.partial(logit_kernel, latent, n_head),
        in_specs=[SMEM, SMEM] + [VMEM] * (2 * n_head + 1 + len(blocks)),
        out_specs=VMEM,
        out_shape=jax.ShapeDtypeStruct((len(blocks) // 2 * rows, 2 * share), jnp.float32),
        scratch_shapes=[
            pltpu.VMEM((n_head * index_here // side, side * share), jnp.float32),
            pltpu.VMEM((len(blocks), rows, idx_width), jnp.bfloat16),
            pltpu.VMEM((len(blocks), rows, share), jnp.float32),
        ],
        cost_estimate=cost(2 * len(blocks) * rows * share * n_head * index_here * idx_width),
        compiler_params=pltpu.CompilerParams(vmem_limit_bytes=LIMIT),
        name="index_logits",
    )(order, live, *parts, *weights, lse, *blocks)


def grad_kernel(latent, first, n_head, order_ref, live_ref, *refs):
    parts, w_refs, masses = refs[:n_head], refs[n_head : 2 * n_head], refs[2 * n_head : 3 * n_head]
    target_ref, w_ref = refs[3 * n_head], refs[-1]
    n_blocks = (len(refs) - 3 * n_head - 2) // 2
    blocks, outs = refs[3 * n_head + 1 : -n_blocks - 1], refs[-n_blocks - 1 : -1]
    rows = blocks[0].shape[1]
    share, idx_width = parts[0].shape[1:]
    scale = 1.0 / idx_width**0.5
    lay_weights(parts, w_refs, w_ref)
    tile = w_ref.shape[1]
    start = lax.axis_index("head") * share
    for i in range(n_blocks):
        later, alive = facts(first + i, order_ref, live_ref)

        @pl.when(alive)
        def _(i=i, later=later):
            here = slice(i // 2 * rows, (i // 2 + 1) * rows)
            span = slice(i % 2 * share, (i % 2 + 1) * share)
            mass = masses[0][here, span]
            for other in masses[1:]:
                mass = mass + other[here, span]
            at = (first + i) // 2 * rows
            value = target_ref[at : at + rows, span] - mass * (1.0 / HEADS)
            within = lax.broadcasted_iota(jnp.int32, (rows, share), 0)
            token = lax.broadcasted_iota(jnp.int32, (rows, share), 1) + start
            grad = jnp.where(within + later * rows <= token, value, 0.0)
            grad = jnp.concatenate([grad] * (tile // share), axis=1)
            held = blocks[i][latent:, :]
            total = jnp.zeros((rows, idx_width), jnp.float32)
            at = 0
            for part in parts:
                for _, run, piece in pieces(part, share, 8):
                    r = lax.dot_general(held, piece, NT, preferred_element_type=jnp.float32)
                    weighted = []
                    for k in range(run):
                        w = grad * w_ref[at + k : at + k + 1, :]
                        w = jnp.where(r[:, k * tile : (k + 1) * tile] > 0.0, w, 0.0)
                        weighted.append(w.astype(jnp.bfloat16))
                    at += run
                    total = total + lax.dot_general(
                        jnp.concatenate(weighted, axis=1),
                        piece,
                        NN,
                        preferred_element_type=jnp.float32,
                    )
            outs[i][...] = total * scale

        @pl.when(jnp.logical_not(alive))
        def _(i=i):
            outs[i][...] = jnp.zeros((rows, idx_width), jnp.float32)


def index_grad(order, live, parts, weights, masses, target, blocks, first, latent):
    n_head, (index_here, share, idx_width) = len(parts), parts[0].shape
    rows = blocks[0].shape[1]
    side = lanes_of(parts[0], share)
    return pl.pallas_call(
        functools.partial(grad_kernel, latent, first, n_head),
        in_specs=[SMEM, SMEM] + [VMEM] * (3 * n_head + 1 + len(blocks)),
        out_specs=[VMEM] * len(blocks),
        out_shape=[jax.ShapeDtypeStruct((rows, idx_width), jnp.float32)] * len(blocks),
        scratch_shapes=[pltpu.VMEM((n_head * index_here // side, side * share), jnp.float32)],
        cost_estimate=cost(4 * len(blocks) * rows * share * n_head * index_here * idx_width),
        compiler_params=pltpu.CompilerParams(vmem_limit_bytes=LIMIT),
        name="index_grad",
    )(order, live, *parts, *weights, *masses, target, *blocks)


def body(
    q_main,
    latent_keys,
    lse_main,
    index_queries,
    index_weights,
    index_keys,
    lse_index,
    slab_order,
    block_live,
):
    n_seq = lax.axis_size("seq")
    n_head = lax.axis_size("head")
    head_place = lax.axis_index("head")
    latent = latent_keys.shape[1]
    share = q_main.shape[0] // n_head
    devices = range(n_seq)

    def ring(distance):
        return [(i, (i + distance) % n_seq) for i in devices]

    def around(array, turn):
        return lax.ppermute(array, "head", [(i, (i + turn) % n_head) for i in range(n_head)])

    forward = [(i, (i + (HOPS - 1 if i % 2 else 1)) % n_seq) for i in devices]
    back = [(b, a) for a, b in forward]
    swap = [(i, i ^ 1) for i in devices]
    own = jnp.concatenate([latent_keys.T, index_keys], axis=0)
    arrived = [lax.ppermute(own, "seq", ring(2))]
    arrived.append(lax.ppermute(own, "seq", ring(4)))
    slots = [own, lax.ppermute(own, "seq", forward)]
    for m in range(1, HOPS // 2):
        if m > 2:
            arrived.append(lax.ppermute(arrived[m - 3], "seq", ring(4)))
        slots += [arrived[m - 1], lax.ppermute(arrived[m - 1], "seq", swap)]

    def to_share(array, turn):
        start = lax.rem(head_place + turn, n_head) * share
        part = lax.dynamic_slice_in_dim(array, start, share, 0)
        return part if turn == 0 else around(part, turn)

    turns = range(n_head)
    weights = [around(index_weights.T, turn) if turn else index_weights.T for turn in turns]
    parts = [to_share(index_queries, turn).transpose(1, 0, 2) for turn in turns]

    tables = slab_order, block_live
    lse = lse_main.T
    early = HOPS - LAST
    q = q_main.transpose(1, 2, 0)
    near = head_mass(*tables, q, lse, slots[:1], [], 0, n_head)
    masses = [
        list(head_mass(*tables, q, lse, slots[1:early], near, 1, n_head)),
        list(head_mass(*tables, q, lse, slots[early:], [], early, n_head)),
    ]
    for group in masses:
        for turn in range(1, n_head):
            group[turn] = around(group[turn], turn)
    target = index_logits(*tables, parts, weights, lse_index[None, :], slots, latent)
    grads = []
    for group, first, end in ((masses[0], 0, early), (masses[1], early, HOPS)):
        grads += index_grad(
            *tables, parts, weights, group, target, slots[first:end], first, latent
        )

    total = grads[0] + lax.ppermute(grads[1], "seq", back)
    for m in range(1, HOPS // 2):
        both = grads[2 * m] + lax.ppermute(grads[2 * m + 1], "seq", swap)
        if n_head == 2 and m == HOPS // 2 - 1:
            break
        total = total + lax.ppermute(both, "seq", ring(-2 * m))
    if n_head != 2:
        return lax.psum(total, "head")
    straight, across = [], []
    for i in devices:
        for x in range(2):
            goal = (i - 2 * m) % n_seq
            straight.append((2 * i + x, 2 * goal + x))
            across.append((2 * i + x, 2 * goal + 1 - x))
    axes = ("seq", "head")
    last = lax.ppermute(both, axes, straight) + lax.ppermute(both, axes, across)
    return total + around(total, 1) + last


def solution(mesh):
    placed = (
        P("seq", "head", None),
        P("seq", None),
        P("seq", "head"),
        P("seq", "head", None),
        P("seq", "head"),
        P("seq", None),
        P("seq"),
        P(),
        P(),
    )
    return jax.shard_map(
        body, mesh=mesh, in_specs=placed, out_specs=P("seq", None), check_vma=False
    )
```

```python
import functools
import math

import jax
import jax.numpy as jnp
from jax import lax
from jax.experimental import pallas as pl
from jax.experimental.pallas import tpu as pltpu
from jax.sharding import PartitionSpec as P


HEADS = 128
HOPS = 8
LAST = 2
LOG2E = math.log2(math.e)
MAIN_SCALE = 1.0 / 192.0**0.5
LIMIT = 20 * 2**20
NT = (((1,), (1,)), ((), ()))
NN = (((1,), (0,)), ((), ()))
VMEM = pl.BlockSpec(memory_space=pltpu.VMEM)
SMEM = pl.BlockSpec(memory_space=pltpu.SMEM)


def facts(slot, order_ref, live_ref):
    n = lax.axis_size("seq")
    me = lax.axis_index("seq")
    crossed = (slot % 2 == 1) & (me % 2 == 0)
    hop = jnp.where(crossed, jnp.where(slot == 1, HOPS - 1, slot - 2), slot)
    own = order_ref[me]
    slab = order_ref[lax.rem(me - hop + n, n)]
    return slab - own, (slab <= own) & (live_ref[own, slab] == 1)


def packed(first, n, order_ref, live_ref):
    count, slots = jnp.int32(0), []
    for i in range(n):
        later, alive = facts(first + i, order_ref, live_ref)
        slots.append((count, later, alive))
        count = count + alive.astype(jnp.int32)
    return slots, count


def at(place, rows, blocks=1):
    return pl.ds(pl.multiple_of(place * rows, rows), blocks * rows)


def in_pairs(count, rows, work):
    def two(i, carry):
        work(at(2 * i, rows, 2))
        return carry

    lax.fori_loop(0, count // 2, two, 0)

    @pl.when(count % 2 == 1)
    def _():
        work(at(count - 1, rows))


def cost(flops):
    return pl.CostEstimate(flops=flops, transcendentals=0, bytes_accessed=flops // 256)


def score_kernel(first, n_blocks, n_head, order_ref, live_ref, q_ref, lse_ref, *refs):
    n_outs = n_head if n_blocks > 1 else 1
    blocks, known = refs[:n_blocks], refs[n_blocks : -n_outs - 2]
    outs, (keys, mass) = refs[-n_outs - 2 : -2], refs[-2:]
    heads, latent, tokens = q_ref.shape
    rows = blocks[0].shape[1]
    slots, count = packed(first, n_blocks, order_ref, live_ref)
    for block, (place, _, alive) in zip(blocks, slots):

        @pl.when(alive)
        def _(block=block, place=place):
            keys[at(place, rows), :] = block[:latent, :].T

    def work(here):
        held = keys[here, :]
        total = None
        for h in range(0, heads, 2):
            pair = jnp.concatenate([q_ref[h], q_ref[h + 1]], axis=1)
            s = lax.dot_general(held, pair, NN, preferred_element_type=jnp.float32)
            s = s * (MAIN_SCALE * LOG2E)
            for n in range(2):
                lse = lse_ref[h + n : h + n + 1, :] * LOG2E
                p = jnp.exp2(s[:, n * tokens : (n + 1) * tokens] - lse)
                total = p if total is None else total + p
        mass[here, :] = total

    in_pairs(count, rows, work)
    values = [ref[...] for ref in known]
    values += [jnp.where(alive, mass[at(place, rows), :], 0.0) for place, _, alive in slots]
    if len(values) == 1:
        outs[0][...] = values[0]
        return
    share = tokens // n_head
    if n_head > 1:
        turn = tokens - lax.axis_index("head") * share
        values = [pltpu.roll(value, turn, 1) for value in values]
    for c in range(len(values) // 2):
        for n, out in enumerate(outs):
            pair = [value[:, n * share : (n + 1) * share] for value in values[2 * c : 2 * c + 2]]
            out[c * rows : (c + 1) * rows, :] = jnp.concatenate(pair, axis=1)


def head_mass(order, live, q, lse, blocks, known, first, n_head):
    heads, latent, tokens = q.shape
    n, rows = len(blocks), blocks[0].shape[1]
    total = n + len(known)
    shapes = [jax.ShapeDtypeStruct((total // 2 * rows, 2 * tokens // n_head), jnp.float32)] * n_head
    if total == 1:
        shapes = [jax.ShapeDtypeStruct((rows, tokens), jnp.float32)]
    return pl.pallas_call(
        functools.partial(score_kernel, first, n, n_head),
        in_specs=[SMEM, SMEM] + [VMEM] * (2 + total),
        out_specs=[VMEM] * len(shapes),
        out_shape=shapes,
        scratch_shapes=[
            pltpu.VMEM((n * rows, latent), jnp.bfloat16),
            pltpu.VMEM((n * rows, tokens), jnp.float32),
        ],
        cost_estimate=cost(2 * tokens * heads * latent * n * rows),
        compiler_params=pltpu.CompilerParams(vmem_limit_bytes=LIMIT),
        name="score_mass",
    )(order, live, q, lse, *blocks, *known)


def lanes_of(part, share):
    return max(1, min(part.shape[0], 128 // share))


def pieces(part, share, width):
    side = lanes_of(part, share)
    step = part.shape[0] // side
    run = max(1, min(step, width))
    for first in range(0, step, run):
        heads = [part[k + n * step] for k in range(first, first + run) for n in range(side)]
        yield run, jnp.concatenate(heads, axis=0)


def lay_weights(parts, w_refs, w_lanes):
    row = 0
    for part, w_ref in zip(parts, w_refs):
        index_here, tokens = w_ref.shape
        share = part.shape[1]
        w = w_ref[...]
        if share < tokens:
            w = pltpu.roll(w, tokens - lax.axis_index("head") * share, 1)
        side = lanes_of(part, share)
        step = index_here // side
        tile = [w[n * step : (n + 1) * step, :share] for n in range(side)]
        w_lanes[row : row + step, :] = jnp.concatenate(tile, axis=1)
        row += step


def logit_kernel(latent, n_head, order_ref, live_ref, *refs):
    parts, w_refs, lse_ref = refs[:n_head], refs[n_head : 2 * n_head], refs[2 * n_head]
    blocks, (out_ref, w_ref, keys, values) = refs[2 * n_head + 1 : -4], refs[-4:]
    rows, idx_width = blocks[0].shape[1], keys.shape[1]
    share = parts[0].shape[1]
    scale = 1.0 / idx_width**0.5
    lay_weights(parts, w_refs, w_ref)
    tile = w_ref.shape[1]
    lse = lse_ref[...]
    if share < lse.shape[1]:
        lse = pltpu.roll(lse, lse.shape[1] - lax.axis_index("head") * share, 1)[:, :share]
    slots, count = packed(0, len(blocks), order_ref, live_ref)
    for block, (place, _, alive) in zip(blocks, slots):

        @pl.when(alive)
        def _(block=block, place=place):
            keys[at(place, rows), :] = block[latent:, :]

    def work(here):
        held = keys[here, :]
        acc = jnp.zeros((held.shape[0], tile), jnp.float32)
        row = 0
        for part in parts:
            for run, piece in pieces(part, share, 8):
                r = lax.dot_general(held, piece, NT, preferred_element_type=jnp.float32)
                for k in range(run):
                    relu = jnp.maximum(r[:, k * tile : (k + 1) * tile], 0.0)
                    acc = acc + relu * w_ref[row + k : row + k + 1, :]
                row += run
        logits = acc[:, :share]
        for first in range(share, tile, share):
            logits = logits + acc[:, first : first + share]
        values[here, :] = jnp.exp(logits * scale - lse)

    in_pairs(count, rows, work)
    for c in range(len(blocks) // 2):
        pair = [jnp.where(s[2], values[at(s[0], rows), :], 0.0) for s in slots[2 * c : 2 * c + 2]]
        out_ref[c * rows : (c + 1) * rows, :] = jnp.concatenate(pair, axis=1)


def index_logits(order, live, parts, weights, lse, blocks, latent):
    n_head, (index_here, share, idx_width) = len(parts), parts[0].shape
    rows = blocks[0].shape[1]
    side = lanes_of(parts[0], share)
    return pl.pallas_call(
        functools.partial(logit_kernel, latent, n_head),
        in_specs=[SMEM, SMEM] + [VMEM] * (2 * n_head + 1 + len(blocks)),
        out_specs=VMEM,
        out_shape=jax.ShapeDtypeStruct((len(blocks) // 2 * rows, 2 * share), jnp.float32),
        scratch_shapes=[
            pltpu.VMEM((n_head * index_here // side, side * share), jnp.float32),
            pltpu.VMEM((len(blocks) * rows, idx_width), jnp.bfloat16),
            pltpu.VMEM((len(blocks) * rows, share), jnp.float32),
        ],
        cost_estimate=cost(2 * len(blocks) * rows * share * n_head * index_here * idx_width),
        compiler_params=pltpu.CompilerParams(vmem_limit_bytes=LIMIT),
        name="index_logits",
    )(order, live, *parts, *weights, lse, *blocks)


def grad_kernel(latent, first, n_head, order_ref, live_ref, *refs):
    parts, w_refs, masses = refs[:n_head], refs[n_head : 2 * n_head], refs[2 * n_head : 3 * n_head]
    target_ref, (w_ref, keys, grads, results) = refs[3 * n_head], refs[-4:]
    n_blocks = (len(refs) - 3 * n_head - 5) // 2
    blocks, outs = refs[3 * n_head + 1 : -n_blocks - 4], refs[-n_blocks - 4 : -4]
    rows = blocks[0].shape[1]
    share, idx_width = parts[0].shape[1:]
    scale = 1.0 / idx_width**0.5
    lay_weights(parts, w_refs, w_ref)
    tile = w_ref.shape[1]
    start = lax.axis_index("head") * share
    slots, count = packed(first, n_blocks, order_ref, live_ref)
    for i, (place, later, alive) in enumerate(slots):

        @pl.when(alive)
        def _(i=i, place=place, later=later):
            here = slice(i // 2 * rows, (i // 2 + 1) * rows)
            span = slice(i % 2 * share, (i % 2 + 1) * share)
            mass = masses[0][here, span]
            for other in masses[1:]:
                mass = mass + other[here, span]
            there = (first + i) // 2 * rows
            value = target_ref[there : there + rows, span] - mass * (1.0 / HEADS)
            within = lax.broadcasted_iota(jnp.int32, (rows, share), 0)
            token = lax.broadcasted_iota(jnp.int32, (rows, share), 1) + start
            grad = jnp.where(within + later * rows <= token, value, 0.0)
            grads[at(place, rows), :] = jnp.concatenate([grad] * (tile // share), axis=1)
            keys[at(place, rows), :] = blocks[i][latent:, :]

    def work(here):
        held = keys[here, :]
        grad = grads[here, :]
        total = jnp.zeros((held.shape[0], idx_width), jnp.float32)
        row = 0
        for part in parts:
            for run, piece in pieces(part, share, 8):
                r = lax.dot_general(held, piece, NT, preferred_element_type=jnp.float32)
                weighted = []
                for k in range(run):
                    w = grad * w_ref[row + k : row + k + 1, :]
                    w = jnp.where(r[:, k * tile : (k + 1) * tile] > 0.0, w, 0.0)
                    weighted.append(w.astype(jnp.bfloat16))
                row += run
                total = total + lax.dot_general(
                    jnp.concatenate(weighted, axis=1), piece, NN, preferred_element_type=jnp.float32
                )
        results[here, :] = total * scale

    in_pairs(count, rows, work)
    for out, (place, _, alive) in zip(outs, slots):
        out[...] = jnp.where(alive, results[at(place, rows), :], 0.0)


def index_grad(order, live, parts, weights, masses, target, blocks, first, latent):
    n_head, (index_here, share, idx_width) = len(parts), parts[0].shape
    rows = blocks[0].shape[1]
    side = lanes_of(parts[0], share)
    return pl.pallas_call(
        functools.partial(grad_kernel, latent, first, n_head),
        in_specs=[SMEM, SMEM] + [VMEM] * (3 * n_head + 1 + len(blocks)),
        out_specs=[VMEM] * len(blocks),
        out_shape=[jax.ShapeDtypeStruct((rows, idx_width), jnp.float32)] * len(blocks),
        scratch_shapes=[
            pltpu.VMEM((n_head * index_here // side, side * share), jnp.float32),
            pltpu.VMEM((len(blocks) * rows, idx_width), jnp.bfloat16),
            pltpu.VMEM((len(blocks) * rows, side * share), jnp.float32),
            pltpu.VMEM((len(blocks) * rows, idx_width), jnp.float32),
        ],
        cost_estimate=cost(4 * len(blocks) * rows * share * n_head * index_here * idx_width),
        compiler_params=pltpu.CompilerParams(vmem_limit_bytes=LIMIT),
        name="index_grad",
    )(order, live, *parts, *weights, *masses, target, *blocks)


def body(
    q_main,
    latent_keys,
    lse_main,
    index_queries,
    index_weights,
    index_keys,
    lse_index,
    slab_order,
    block_live,
):
    n_seq = lax.axis_size("seq")
    n_head = lax.axis_size("head")
    head_place = lax.axis_index("head")
    latent = latent_keys.shape[1]
    share = q_main.shape[0] // n_head
    devices = range(n_seq)

    def ring(distance):
        return [(i, (i + distance) % n_seq) for i in devices]

    def around(array, turn):
        return lax.ppermute(array, "head", [(i, (i + turn) % n_head) for i in range(n_head)])

    forward = [(i, (i + (HOPS - 1 if i % 2 else 1)) % n_seq) for i in devices]
    back = [(b, a) for a, b in forward]
    swap = [(i, i ^ 1) for i in devices]
    own = jnp.concatenate([latent_keys.T, index_keys], axis=0)
    arrived = [lax.ppermute(own, "seq", ring(2))]
    arrived.append(lax.ppermute(own, "seq", ring(4)))
    slots = [own, lax.ppermute(own, "seq", forward)]
    for m in range(1, HOPS // 2):
        if m > 2:
            arrived.append(lax.ppermute(arrived[m - 3], "seq", ring(4)))
        slots += [arrived[m - 1], lax.ppermute(arrived[m - 1], "seq", swap)]

    def to_share(array, turn):
        start = lax.rem(head_place + turn, n_head) * share
        part = lax.dynamic_slice_in_dim(array, start, share, 0)
        return part if turn == 0 else around(part, turn)

    turns = range(n_head)
    weights = [around(index_weights.T, turn) if turn else index_weights.T for turn in turns]
    parts = [to_share(index_queries, turn).transpose(1, 0, 2) for turn in turns]

    tables = slab_order, block_live
    lse = lse_main.T
    early = HOPS - LAST
    q = q_main.transpose(1, 2, 0)
    own_mass = head_mass(*tables, q, lse, slots[:1], [], 0, n_head)
    masses = [
        list(head_mass(*tables, q, lse, slots[1:early], own_mass, 1, n_head)),
        list(head_mass(*tables, q, lse, slots[early:], [], early, n_head)),
    ]
    for group in masses:
        for turn in range(1, n_head):
            group[turn] = around(group[turn], turn)
    target = index_logits(*tables, parts, weights, lse_index[None, :], slots, latent)
    grads = []
    for group, (first, end) in zip(masses, ((0, early), (early, HOPS))):
        blocks = slots[first:end]
        grads += index_grad(*tables, parts, weights, group, target, blocks, first, latent)

    total = grads[0] + lax.ppermute(grads[1], "seq", back)
    for m in range(1, HOPS // 2):
        both = grads[2 * m] + lax.ppermute(grads[2 * m + 1], "seq", swap)
        if n_head == 2 and m == HOPS // 2 - 1:
            break
        total = total + lax.ppermute(both, "seq", ring(-2 * m))
    if n_head != 2:
        return lax.psum(total, "head")
    straight, across = [], []
    for i in devices:
        for x in range(2):
            goal = (i - 2 * m) % n_seq
            straight.append((2 * i + x, 2 * goal + x))
            across.append((2 * i + x, 2 * goal + 1 - x))
    axes = ("seq", "head")
    last = lax.ppermute(both, axes, straight) + lax.ppermute(both, axes, across)
    return total + around(total, 1) + last


def solution(mesh):
    placed = (
        P("seq", "head", None),
        P("seq", None),
        P("seq", "head"),
        P("seq", "head", None),
        P("seq", "head"),
        P("seq", None),
        P("seq"),
        P(),
        P(),
    )
    return jax.shard_map(
        body, mesh=mesh, in_specs=placed, out_specs=P("seq", None), check_vma=False
    )
```

```python
import functools
import math

import jax
import jax.numpy as jnp
from jax import lax
from jax.experimental import pallas as pl
from jax.experimental.pallas import tpu as pltpu
from jax.sharding import PartitionSpec as P


HEADS = 128
HOPS = 8
LOG2E = math.log2(math.e)
MAIN_SCALE = 1.0 / 192.0**0.5
LIMIT = 20 * 2**20
NT = (((1,), (1,)), ((), ()))
NN = (((1,), (0,)), ((), ()))
VMEM = pl.BlockSpec(memory_space=pltpu.VMEM)
SMEM = pl.BlockSpec(memory_space=pltpu.SMEM)


def facts(slot, order_ref, live_ref):
    n = lax.axis_size("seq")
    me = lax.axis_index("seq")
    crossed = (slot % 2 == 1) & (me % 2 == 0)
    hop = jnp.where(crossed, jnp.where(slot == 1, HOPS - 1, slot - 2), slot)
    own = order_ref[me]
    slab = order_ref[lax.rem(me - hop + n, n)]
    return slab - own, (slab <= own) & (live_ref[own, slab] == 1)


def packed(ids, order_ref, live_ref):
    count, slots = jnp.int32(0), []
    for i in ids:
        later, alive = facts(i, order_ref, live_ref)
        slots.append((count, later, alive))
        count = count + alive.astype(jnp.int32)
    return slots, count


def side_by_side(values):
    if len(values) % 2:
        values = values + [jnp.zeros_like(values[0])]
    pairs = [jnp.concatenate(values[i : i + 2], axis=1) for i in range(0, len(values), 2)]
    return jnp.concatenate(pairs, axis=0)


def side_by_side_shape(n, rows, share):
    return jax.ShapeDtypeStruct(((n + 1) // 2 * rows, 2 * share), jnp.float32)


def at(place, rows, blocks=1):
    return pl.ds(pl.multiple_of(place * rows, rows), blocks * rows)


def in_pairs(count, rows, work):
    def two(i, carry):
        work(at(2 * i, rows, 2))
        return carry

    lax.fori_loop(0, count // 2, two, 0)

    @pl.when(count % 2 == 1)
    def _():
        work(at(count - 1, rows))


def cost(flops):
    return pl.CostEstimate(flops=flops, transcendentals=0, bytes_accessed=flops // 256)


def score_kernel(ids, n_outs, pack, order_ref, live_ref, q_ref, lse_ref, *refs):
    blocks, known = refs[: len(ids)], refs[len(ids) : -n_outs - 2]
    outs, (keys, mass) = refs[-n_outs - 2 : -2], refs[-2:]
    heads, latent, tokens = q_ref.shape
    rows = blocks[0].shape[1]
    slots, count = packed(ids, order_ref, live_ref)
    for block, (place, _, alive) in zip(blocks, slots):

        @pl.when(alive)
        def _(block=block, place=place):
            keys[at(place, rows), :] = block[:latent, :].T

    def work(here):
        held = keys[here, :]
        total = None
        for h in range(0, heads, 2):
            pair = jnp.concatenate([q_ref[h], q_ref[h + 1]], axis=1)
            s = lax.dot_general(held, pair, NN, preferred_element_type=jnp.float32)
            s = s * (MAIN_SCALE * LOG2E)
            for n in range(2):
                lse = lse_ref[h + n : h + n + 1, :] * LOG2E
                p = jnp.exp2(s[:, n * tokens : (n + 1) * tokens] - lse)
                total = p if total is None else total + p
        mass[here, :] = total

    in_pairs(count, rows, work)
    values = [jnp.where(alive, mass[at(place, rows), :], 0.0) for place, _, alive in slots]
    if not pack:
        for out, value in zip(outs, values):
            out[...] = value
        return
    values = [ref[...] for ref in known] + values
    share = tokens // n_outs
    if n_outs > 1:
        turn = tokens - lax.axis_index("head") * share
        values = [pltpu.roll(value, turn, 1) for value in values]
    for n, out in enumerate(outs):
        out[...] = side_by_side([value[:, n * share : (n + 1) * share] for value in values])


def head_mass(tables, q, lse, ids, blocks, known=(), n_head=0):
    heads, latent, tokens = q.shape
    n, rows = len(ids), blocks[0].shape[1]
    shapes = [jax.ShapeDtypeStruct((rows, tokens), jnp.float32)] * n
    if n_head:
        shapes = [side_by_side_shape(n + len(known), rows, tokens // n_head)] * n_head
    return pl.pallas_call(
        functools.partial(score_kernel, ids, len(shapes), n_head > 0),
        in_specs=[SMEM, SMEM] + [VMEM] * (2 + n + len(known)),
        out_specs=[VMEM] * len(shapes),
        out_shape=shapes,
        scratch_shapes=[
            pltpu.VMEM((n * rows, latent), jnp.bfloat16),
            pltpu.VMEM((n * rows, tokens), jnp.float32),
        ],
        cost_estimate=cost(2 * tokens * heads * latent * n * rows),
        compiler_params=pltpu.CompilerParams(vmem_limit_bytes=LIMIT),
        name="score_mass",
    )(*tables, q, lse, *blocks, *known)


def lanes_of(part, share):
    return max(1, min(part.shape[0], 128 // share))


def pieces(part, share, width):
    side = lanes_of(part, share)
    step = part.shape[0] // side
    run = max(1, min(step, width))
    for first in range(0, step, run):
        heads = [part[k + n * step] for k in range(first, first + run) for n in range(side)]
        yield run, jnp.concatenate(heads, axis=0)


def lay_weights(parts, w_refs, w_lanes):
    row = 0
    for part, w_ref in zip(parts, w_refs):
        index_here, tokens = w_ref.shape
        share = part.shape[1]
        w = w_ref[...]
        if share < tokens:
            w = pltpu.roll(w, tokens - lax.axis_index("head") * share, 1)
        side = lanes_of(part, share)
        step = index_here // side
        tile = [w[n * step : (n + 1) * step, :share] for n in range(side)]
        w_lanes[row : row + step, :] = jnp.concatenate(tile, axis=1)
        row += step


def logit_kernel(latent, ids, n_head, order_ref, live_ref, *refs):
    parts, w_refs, lse_ref = refs[:n_head], refs[n_head : 2 * n_head], refs[2 * n_head]
    blocks, (out_ref, w_ref, keys, values) = refs[2 * n_head + 1 : -4], refs[-4:]
    rows, idx_width = blocks[0].shape[1], keys.shape[1]
    share = parts[0].shape[1]
    scale = 1.0 / idx_width**0.5
    lay_weights(parts, w_refs, w_ref)
    tile = w_ref.shape[1]
    lse = lse_ref[...]
    if share < lse.shape[1]:
        lse = pltpu.roll(lse, lse.shape[1] - lax.axis_index("head") * share, 1)[:, :share]
    slots, count = packed(ids, order_ref, live_ref)
    for block, (place, _, alive) in zip(blocks, slots):

        @pl.when(alive)
        def _(block=block, place=place):
            keys[at(place, rows), :] = block[latent:, :]

    def work(here):
        held = keys[here, :]
        acc = jnp.zeros((held.shape[0], tile), jnp.float32)
        row = 0
        for part in parts:
            for run, piece in pieces(part, share, 8):
                r = lax.dot_general(held, piece, NT, preferred_element_type=jnp.float32)
                for k in range(run):
                    relu = jnp.maximum(r[:, k * tile : (k + 1) * tile], 0.0)
                    acc = acc + relu * w_ref[row + k : row + k + 1, :]
                row += run
        logits = acc[:, :share]
        for first in range(share, tile, share):
            logits = logits + acc[:, first : first + share]
        values[here, :] = jnp.exp(logits * scale - lse)

    in_pairs(count, rows, work)
    out_ref[...] = side_by_side([jnp.where(s[2], values[at(s[0], rows), :], 0.0) for s in slots])


def index_logits(tables, parts, weights, lse, ids, blocks, latent):
    n_head, (index_here, share, idx_width) = len(parts), parts[0].shape
    rows = blocks[0].shape[1]
    side = lanes_of(parts[0], share)
    return pl.pallas_call(
        functools.partial(logit_kernel, latent, ids, n_head),
        in_specs=[SMEM, SMEM] + [VMEM] * (2 * n_head + 1 + len(blocks)),
        out_specs=VMEM,
        out_shape=side_by_side_shape(len(blocks), rows, share),
        scratch_shapes=[
            pltpu.VMEM((n_head * index_here // side, side * share), jnp.float32),
            pltpu.VMEM((len(blocks) * rows, idx_width), jnp.bfloat16),
            pltpu.VMEM((len(blocks) * rows, share), jnp.float32),
        ],
        cost_estimate=cost(2 * len(blocks) * rows * share * n_head * index_here * idx_width),
        compiler_params=pltpu.CompilerParams(vmem_limit_bytes=LIMIT),
        name="index_logits",
    )(*tables, *parts, *weights, lse, *blocks)


def grad_kernel(latent, ids, n_head, order_ref, live_ref, *refs):
    parts, w_refs, masses = refs[:n_head], refs[n_head : 2 * n_head], refs[2 * n_head : 3 * n_head]
    target_ref, (w_ref, keys, grads, results) = refs[3 * n_head], refs[-4:]
    n_blocks = (len(refs) - 3 * n_head - 5) // 2
    blocks, outs = refs[3 * n_head + 1 : -n_blocks - 4], refs[-n_blocks - 4 : -4]
    rows = blocks[0].shape[1]
    share, idx_width = parts[0].shape[1:]
    scale = 1.0 / idx_width**0.5
    lay_weights(parts, w_refs, w_ref)
    tile = w_ref.shape[1]
    start = lax.axis_index("head") * share
    slots, count = packed(ids, order_ref, live_ref)
    for i, (place, later, alive) in enumerate(slots):

        @pl.when(alive)
        def _(i=i, place=place, later=later):
            here = slice(i // 2 * rows, (i // 2 + 1) * rows)
            span = slice(i % 2 * share, (i % 2 + 1) * share)
            mass = masses[0][here, span]
            for other in masses[1:]:
                mass = mass + other[here, span]
            value = target_ref[here, span] - mass * (1.0 / HEADS)
            within = lax.broadcasted_iota(jnp.int32, (rows, share), 0)
            token = lax.broadcasted_iota(jnp.int32, (rows, share), 1) + start
            grad = jnp.where(within + later * rows <= token, value, 0.0)
            grads[at(place, rows), :] = jnp.concatenate([grad] * (tile // share), axis=1)
            keys[at(place, rows), :] = blocks[i][latent:, :]

    def work(here):
        held = keys[here, :]
        grad = grads[here, :]
        total = jnp.zeros((held.shape[0], idx_width), jnp.float32)
        row = 0
        for part in parts:
            for run, piece in pieces(part, share, 8):
                r = lax.dot_general(held, piece, NT, preferred_element_type=jnp.float32)
                weighted = []
                for k in range(run):
                    w = grad * w_ref[row + k : row + k + 1, :]
                    w = jnp.where(r[:, k * tile : (k + 1) * tile] > 0.0, w, 0.0)
                    weighted.append(w.astype(jnp.bfloat16))
                row += run
                total = total + lax.dot_general(
                    jnp.concatenate(weighted, axis=1), piece, NN, preferred_element_type=jnp.float32
                )
        results[here, :] = total * scale

    in_pairs(count, rows, work)
    for out, (place, _, alive) in zip(outs, slots):
        out[...] = jnp.where(alive, results[at(place, rows), :], 0.0)


def index_grad(tables, parts, weights, masses, target, ids, blocks, latent):
    n_head, (index_here, share, idx_width) = len(parts), parts[0].shape
    rows = blocks[0].shape[1]
    side = lanes_of(parts[0], share)
    return pl.pallas_call(
        functools.partial(grad_kernel, latent, ids, n_head),
        in_specs=[SMEM, SMEM] + [VMEM] * (3 * n_head + 1 + len(blocks)),
        out_specs=[VMEM] * len(blocks),
        out_shape=[jax.ShapeDtypeStruct((rows, idx_width), jnp.float32)] * len(blocks),
        scratch_shapes=[
            pltpu.VMEM((n_head * index_here // side, side * share), jnp.float32),
            pltpu.VMEM((len(blocks) * rows, idx_width), jnp.bfloat16),
            pltpu.VMEM((len(blocks) * rows, side * share), jnp.float32),
            pltpu.VMEM((len(blocks) * rows, idx_width), jnp.float32),
        ],
        cost_estimate=cost(4 * len(blocks) * rows * share * n_head * index_here * idx_width),
        compiler_params=pltpu.CompilerParams(vmem_limit_bytes=LIMIT),
        name="index_grad",
    )(*tables, *parts, *weights, *masses, target, *blocks)


def body(
    q_main,
    latent_keys,
    lse_main,
    index_queries,
    index_weights,
    index_keys,
    lse_index,
    slab_order,
    block_live,
):
    n_seq = lax.axis_size("seq")
    n_head = lax.axis_size("head")
    head_place = lax.axis_index("head")
    latent = latent_keys.shape[1]
    share = q_main.shape[0] // n_head
    devices = range(n_seq)

    def ring(distance):
        return [(i, (i + distance) % n_seq) for i in devices]

    def around(array, turn):
        return lax.ppermute(array, "head", [(i, (i + turn) % n_head) for i in range(n_head)])

    forward = [(i, (i + (HOPS - 1 if i % 2 else 1)) % n_seq) for i in devices]
    back = [(b, a) for a, b in forward]
    swap = [(i, i ^ 1) for i in devices]
    own = jnp.concatenate([latent_keys.T, index_keys], axis=0)
    arrived = [lax.ppermute(own, "seq", ring(2))]
    arrived.append(lax.ppermute(own, "seq", ring(4)))
    slots = [own, lax.ppermute(own, "seq", forward)]
    for m in range(1, HOPS // 2):
        if m > 2:
            arrived.append(lax.ppermute(arrived[m - 3], "seq", ring(4)))
        slots += [arrived[m - 1], lax.ppermute(arrived[m - 1], "seq", swap)]

    def to_share(array, turn):
        start = lax.rem(head_place + turn, n_head) * share
        part = lax.dynamic_slice_in_dim(array, start, share, 0)
        return part if turn == 0 else around(part, turn)

    turns = range(n_head)
    weights = [around(index_weights.T, turn) if turn else index_weights.T for turn in turns]
    parts = [to_share(index_queries, turn).transpose(1, 0, 2) for turn in turns]

    tables = slab_order, block_live
    q, lse, lse_share = q_main.transpose(1, 2, 0), lse_main.T, lse_index[None, :]

    def blocks(ids):
        return [slots[i] for i in ids]

    runs = [(0,)] + [(2 * m, 2 * m + 1) for m in range(1, HOPS // 2 - 1)]
    runs[-1] += (1,)
    early = tuple(i for run in runs for i in run)
    late = (HOPS - 2, HOPS - 1)
    known = []
    for run in runs[:-1]:
        known += head_mass(tables, q, lse, run, blocks(run))
    group = head_mass(tables, q, lse, runs[-1], blocks(runs[-1]), known, n_head)
    masses = [list(group)]
    masses.append(list(head_mass(tables, q, lse, late, blocks(late), (), n_head)))
    grads = {}
    for ids, mass in zip((early, late), masses):
        for turn in range(1, n_head):
            mass[turn] = around(mass[turn], turn)
        target = index_logits(tables, parts, weights, lse_share, ids, blocks(ids), latent)
        found = index_grad(tables, parts, weights, mass, target, ids, blocks(ids), latent)
        grads.update(zip(ids, found))

    total = grads[0] + lax.ppermute(grads[1], "seq", back)
    for m in range(1, HOPS // 2):
        both = grads[2 * m] + lax.ppermute(grads[2 * m + 1], "seq", swap)
        if m < HOPS // 2 - 1:
            total = total + lax.ppermute(both, "seq", ring(-2 * m))
    if n_head != 2:
        return lax.psum(total + lax.ppermute(both, "seq", ring(-2 * m)), "head")
    last = []
    for turn in range(2):
        route = [
            (2 * i + x, 2 * ((i - 2 * m) % n_seq) + (x + turn) % 2) for i in devices for x in range(2)
        ]
        last.append(lax.ppermute(both, ("seq", "head"), route))
    total = total + around(total, 1)
    return total + (last[0] + last[1])


def solution(mesh):
    placed = (
        P("seq", "head", None),
        P("seq", None),
        P("seq", "head"),
        P("seq", "head", None),
        P("seq", "head"),
        P("seq", None),
        P("seq"),
        P(),
        P(),
    )
    return jax.shard_map(
        body, mesh=mesh, in_specs=placed, out_specs=P("seq", None), check_vma=False
    )
```

```python
import functools
import math

import jax
import jax.numpy as jnp
from jax import lax
from jax.experimental import pallas as pl
from jax.experimental.pallas import tpu as pltpu
from jax.sharding import PartitionSpec as P


HEADS = 128
HOPS = 8
LOG2E = math.log2(math.e)
MAIN_SCALE = 1.0 / 192.0**0.5
LIMIT = 20 * 2**20
PACK_COST = 10**10
NT = (((1,), (1,)), ((), ()))
NN = (((1,), (0,)), ((), ()))
VMEM = pl.BlockSpec(memory_space=pltpu.VMEM)
SMEM = pl.BlockSpec(memory_space=pltpu.SMEM)
HBM = pl.BlockSpec(memory_space=pltpu.HBM)


def pack_kernel(latent_ref, index_ref, queries_ref, block_ref, *rest):
    shares, sems = rest[:-1], rest[-1]
    latent = latent_ref.shape[0]
    rows = index_ref.shape[0]
    n, share = len(shares), shares[0].shape[0]
    copies = [
        (latent_ref, block_ref.at[pl.ds(0, latent)]),
        (index_ref, block_ref.at[pl.ds(latent, rows)]),
    ]
    for turn, out in enumerate(shares):
        start = lax.rem(lax.axis_index("head") + turn, n) * share
        copies.append((queries_ref.at[pl.ds(start, share)], out))
    copies = [pltpu.make_async_copy(a, b, sems.at[i]) for i, (a, b) in enumerate(copies)]
    for copy in copies:
        copy.start()
    for copy in copies:
        copy.wait()


def packed_inputs(latent_keys, index_keys, index_queries, n_head):
    latent, rows = latent_keys.shape
    tokens, index_here, idx_width = index_queries.shape
    share = jax.ShapeDtypeStruct((tokens // n_head, index_here, idx_width), index_queries.dtype)
    block, *shares = pl.pallas_call(
        pack_kernel,
        in_specs=[HBM] * 3,
        out_specs=[VMEM] * (1 + n_head),
        out_shape=[jax.ShapeDtypeStruct((latent + rows, rows), latent_keys.dtype)] + [share] * n_head,
        scratch_shapes=[pltpu.SemaphoreType.DMA((2 + n_head,))],
        cost_estimate=cost(PACK_COST),
        compiler_params=pltpu.CompilerParams(vmem_limit_bytes=LIMIT),
        name="pack_keys",
    )(latent_keys, index_keys, index_queries)
    return block, shares


def facts(slot, order_ref, live_ref):
    n = lax.axis_size("seq")
    me = lax.axis_index("seq")
    crossed = (slot % 2 == 1) & (me % 2 == 0)
    hop = jnp.where(crossed, jnp.where(slot == 1, HOPS - 1, slot - 2), slot)
    own = order_ref[me]
    slab = order_ref[lax.rem(me - hop + n, n)]
    return slab - own, (slab <= own) & (live_ref[own, slab] == 1)


def packed(ids, order_ref, live_ref):
    count, slots = jnp.int32(0), []
    for i in ids:
        later, alive = facts(i, order_ref, live_ref)
        slots.append((count, later, alive))
        count = count + alive.astype(jnp.int32)
    return slots, count


def side_by_side(values):
    if len(values) % 2:
        values = values + [jnp.zeros_like(values[0])]
    pairs = [jnp.concatenate(values[i : i + 2], axis=1) for i in range(0, len(values), 2)]
    return jnp.concatenate(pairs, axis=0)


def side_by_side_shape(n, rows, share):
    return jax.ShapeDtypeStruct(((n + 1) // 2 * rows, 2 * share), jnp.float32)


def at(place, rows, blocks=1):
    return pl.ds(pl.multiple_of(place * rows, rows), blocks * rows)


def in_pairs(count, rows, work):
    def two(i, carry):
        work(at(2 * i, rows, 2))
        return carry

    lax.fori_loop(0, count // 2, two, 0)

    @pl.when(count % 2 == 1)
    def _():
        work(at(count - 1, rows))


def cost(flops):
    return pl.CostEstimate(flops=flops, transcendentals=0, bytes_accessed=flops // 256)


def score_kernel(ids, n_outs, pack, order_ref, live_ref, q_ref, lse_ref, *refs):
    blocks, known = refs[: len(ids)], refs[len(ids) : -n_outs - 2]
    outs, (keys, mass) = refs[-n_outs - 2 : -2], refs[-2:]
    heads, latent, tokens = q_ref.shape
    rows = blocks[0].shape[1]
    slots, count = packed(ids, order_ref, live_ref)
    for block, (place, _, alive) in zip(blocks, slots):

        @pl.when(alive)
        def _(block=block, place=place):
            keys[at(place, rows), :] = block[:latent, :].T

    def work(here):
        held = keys[here, :]
        total = None
        for h in range(0, heads, 2):
            pair = jnp.concatenate([q_ref[h], q_ref[h + 1]], axis=1)
            s = lax.dot_general(held, pair, NN, preferred_element_type=jnp.float32)
            s = s * (MAIN_SCALE * LOG2E)
            for n in range(2):
                lse = lse_ref[h + n : h + n + 1, :] * LOG2E
                p = jnp.exp2(s[:, n * tokens : (n + 1) * tokens] - lse)
                total = p if total is None else total + p
        mass[here, :] = total

    in_pairs(count, rows, work)
    values = [jnp.where(alive, mass[at(place, rows), :], 0.0) for place, _, alive in slots]
    if not pack:
        for out, value in zip(outs, values):
            out[...] = value
        return
    values = [ref[...] for ref in known] + values
    share = tokens // n_outs
    if n_outs > 1:
        turn = tokens - lax.axis_index("head") * share
        values = [pltpu.roll(value, turn, 1) for value in values]
    for n, out in enumerate(outs):
        out[...] = side_by_side([value[:, n * share : (n + 1) * share] for value in values])


def head_mass(tables, q, lse, ids, blocks, known=(), n_head=0):
    heads, latent, tokens = q.shape
    n, rows = len(ids), blocks[0].shape[1]
    shapes = [jax.ShapeDtypeStruct((rows, tokens), jnp.float32)] * n
    if n_head:
        shapes = [side_by_side_shape(n + len(known), rows, tokens // n_head)] * n_head
    return pl.pallas_call(
        functools.partial(score_kernel, ids, len(shapes), n_head > 0),
        in_specs=[SMEM, SMEM] + [VMEM] * (2 + n + len(known)),
        out_specs=[VMEM] * len(shapes),
        out_shape=shapes,
        scratch_shapes=[
            pltpu.VMEM((n * rows, latent), jnp.bfloat16),
            pltpu.VMEM((n * rows, tokens), jnp.float32),
        ],
        cost_estimate=cost(2 * tokens * heads * latent * n * rows),
        compiler_params=pltpu.CompilerParams(vmem_limit_bytes=LIMIT),
        name="score_mass",
    )(*tables, q, lse, *blocks, *known)


def lanes_of(part, share):
    return max(1, min(part.shape[0], 128 // share))


def pieces(part, share, width):
    side = lanes_of(part, share)
    step = part.shape[0] // side
    run = max(1, min(step, width))
    for first in range(0, step, run):
        heads = [part[k + n * step] for k in range(first, first + run) for n in range(side)]
        yield run, jnp.concatenate(heads, axis=0)


def lay_weights(parts, w_refs, w_lanes):
    row = 0
    for part, w_ref in zip(parts, w_refs):
        index_here, tokens = w_ref.shape
        share = part.shape[1]
        w = w_ref[...]
        if share < tokens:
            w = pltpu.roll(w, tokens - lax.axis_index("head") * share, 1)
        side = lanes_of(part, share)
        step = index_here // side
        tile = [w[n * step : (n + 1) * step, :share] for n in range(side)]
        w_lanes[row : row + step, :] = jnp.concatenate(tile, axis=1)
        row += step


def logit_kernel(latent, ids, n_head, order_ref, live_ref, *refs):
    parts, w_refs, lse_ref = refs[:n_head], refs[n_head : 2 * n_head], refs[2 * n_head]
    blocks, (out_ref, w_ref, keys, values) = refs[2 * n_head + 1 : -4], refs[-4:]
    rows, idx_width = blocks[0].shape[1], keys.shape[1]
    share = parts[0].shape[1]
    scale = 1.0 / idx_width**0.5
    lay_weights(parts, w_refs, w_ref)
    tile = w_ref.shape[1]
    lse = lse_ref[...]
    if share < lse.shape[1]:
        lse = pltpu.roll(lse, lse.shape[1] - lax.axis_index("head") * share, 1)[:, :share]
    slots, count = packed(ids, order_ref, live_ref)
    for block, (place, _, alive) in zip(blocks, slots):

        @pl.when(alive)
        def _(block=block, place=place):
            keys[at(place, rows), :] = block[latent:, :]

    def work(here):
        held = keys[here, :]
        acc = jnp.zeros((held.shape[0], tile), jnp.float32)
        row = 0
        for part in parts:
            for run, piece in pieces(part, share, 8):
                r = lax.dot_general(held, piece, NT, preferred_element_type=jnp.float32)
                for k in range(run):
                    relu = jnp.maximum(r[:, k * tile : (k + 1) * tile], 0.0)
                    acc = acc + relu * w_ref[row + k : row + k + 1, :]
                row += run
        logits = acc[:, :share]
        for first in range(share, tile, share):
            logits = logits + acc[:, first : first + share]
        values[here, :] = jnp.exp(logits * scale - lse)

    in_pairs(count, rows, work)
    out_ref[...] = side_by_side([jnp.where(s[2], values[at(s[0], rows), :], 0.0) for s in slots])


def index_logits(tables, parts, weights, lse, ids, blocks, latent):
    n_head, (index_here, share, idx_width) = len(parts), parts[0].shape
    rows = blocks[0].shape[1]
    side = lanes_of(parts[0], share)
    return pl.pallas_call(
        functools.partial(logit_kernel, latent, ids, n_head),
        in_specs=[SMEM, SMEM] + [VMEM] * (2 * n_head + 1 + len(blocks)),
        out_specs=VMEM,
        out_shape=side_by_side_shape(len(blocks), rows, share),
        scratch_shapes=[
            pltpu.VMEM((n_head * index_here // side, side * share), jnp.float32),
            pltpu.VMEM((len(blocks) * rows, idx_width), jnp.bfloat16),
            pltpu.VMEM((len(blocks) * rows, share), jnp.float32),
        ],
        cost_estimate=cost(2 * len(blocks) * rows * share * n_head * index_here * idx_width),
        compiler_params=pltpu.CompilerParams(vmem_limit_bytes=LIMIT),
        name="index_logits",
    )(*tables, *parts, *weights, lse, *blocks)


def grad_kernel(latent, ids, n_head, order_ref, live_ref, *refs):
    parts, w_refs, masses = refs[:n_head], refs[n_head : 2 * n_head], refs[2 * n_head : 3 * n_head]
    target_ref, (w_ref, keys, grads, results) = refs[3 * n_head], refs[-4:]
    n_blocks = (len(refs) - 3 * n_head - 5) // 2
    blocks, outs = refs[3 * n_head + 1 : -n_blocks - 4], refs[-n_blocks - 4 : -4]
    rows = blocks[0].shape[1]
    share, idx_width = parts[0].shape[1:]
    scale = 1.0 / idx_width**0.5
    lay_weights(parts, w_refs, w_ref)
    tile = w_ref.shape[1]
    start = lax.axis_index("head") * share
    slots, count = packed(ids, order_ref, live_ref)
    for i, (place, later, alive) in enumerate(slots):

        @pl.when(alive)
        def _(i=i, place=place, later=later):
            here = slice(i // 2 * rows, (i // 2 + 1) * rows)
            span = slice(i % 2 * share, (i % 2 + 1) * share)
            mass = masses[0][here, span]
            for other in masses[1:]:
                mass = mass + other[here, span]
            value = target_ref[here, span] - mass * (1.0 / HEADS)
            within = lax.broadcasted_iota(jnp.int32, (rows, share), 0)
            token = lax.broadcasted_iota(jnp.int32, (rows, share), 1) + start
            grad = jnp.where(within + later * rows <= token, value, 0.0)
            grads[at(place, rows), :] = jnp.concatenate([grad] * (tile // share), axis=1)
            keys[at(place, rows), :] = blocks[i][latent:, :]

    def work(here):
        held = keys[here, :]
        grad = grads[here, :]
        total = jnp.zeros((held.shape[0], idx_width), jnp.float32)
        row = 0
        for part in parts:
            for run, piece in pieces(part, share, 8):
                r = lax.dot_general(held, piece, NT, preferred_element_type=jnp.float32)
                weighted = []
                for k in range(run):
                    w = grad * w_ref[row + k : row + k + 1, :]
                    w = jnp.where(r[:, k * tile : (k + 1) * tile] > 0.0, w, 0.0)
                    weighted.append(w.astype(jnp.bfloat16))
                row += run
                total = total + lax.dot_general(
                    jnp.concatenate(weighted, axis=1), piece, NN, preferred_element_type=jnp.float32
                )
        results[here, :] = total * scale

    in_pairs(count, rows, work)
    for out, (place, _, alive) in zip(outs, slots):
        out[...] = jnp.where(alive, results[at(place, rows), :], 0.0)


def index_grad(tables, parts, weights, masses, target, ids, blocks, latent):
    n_head, (index_here, share, idx_width) = len(parts), parts[0].shape
    rows = blocks[0].shape[1]
    side = lanes_of(parts[0], share)
    return pl.pallas_call(
        functools.partial(grad_kernel, latent, ids, n_head),
        in_specs=[SMEM, SMEM] + [VMEM] * (3 * n_head + 1 + len(blocks)),
        out_specs=[VMEM] * len(blocks),
        out_shape=[jax.ShapeDtypeStruct((rows, idx_width), jnp.float32)] * len(blocks),
        scratch_shapes=[
            pltpu.VMEM((n_head * index_here // side, side * share), jnp.float32),
            pltpu.VMEM((len(blocks) * rows, idx_width), jnp.bfloat16),
            pltpu.VMEM((len(blocks) * rows, side * share), jnp.float32),
            pltpu.VMEM((len(blocks) * rows, idx_width), jnp.float32),
        ],
        cost_estimate=cost(4 * len(blocks) * rows * share * n_head * index_here * idx_width),
        compiler_params=pltpu.CompilerParams(vmem_limit_bytes=LIMIT),
        name="index_grad",
    )(*tables, *parts, *weights, *masses, target, *blocks)


def body(
    q_main,
    latent_keys,
    lse_main,
    index_queries,
    index_weights,
    index_keys,
    lse_index,
    slab_order,
    block_live,
):
    n_seq = lax.axis_size("seq")
    n_head = lax.axis_size("head")
    latent = latent_keys.shape[1]
    devices = range(n_seq)

    def ring(distance):
        return [(i, (i + distance) % n_seq) for i in devices]

    def around(array, turn):
        return lax.ppermute(array, "head", [(i, (i + turn) % n_head) for i in range(n_head)])

    forward = [(i, (i + (HOPS - 1 if i % 2 else 1)) % n_seq) for i in devices]
    back = [(b, a) for a, b in forward]
    swap = [(i, i ^ 1) for i in devices]
    own, shares = packed_inputs(latent_keys.T, index_keys, index_queries, n_head)
    arrived = [lax.ppermute(own, "seq", ring(2))]
    arrived.append(lax.ppermute(own, "seq", ring(4)))
    slots = [own, lax.ppermute(own, "seq", forward)]
    for m in range(1, HOPS // 2):
        if m > 2:
            arrived.append(lax.ppermute(arrived[m - 3], "seq", ring(4)))
        slots += [arrived[m - 1], lax.ppermute(arrived[m - 1], "seq", swap)]

    turns = range(n_head)
    weights = [around(index_weights.T, turn) if turn else index_weights.T for turn in turns]
    parts = [around(shares[turn], turn) if turn else shares[turn] for turn in turns]
    parts = [part.transpose(1, 0, 2) for part in parts]

    tables = slab_order, block_live
    q, lse, lse_share = q_main.transpose(1, 2, 0), lse_main.T, lse_index[None, :]

    def blocks(ids):
        return [slots[i] for i in ids]

    runs = [(0,)] + [(2 * m, 2 * m + 1) for m in range(1, HOPS // 2 - 1)]
    runs[-1] += (1,)
    early = tuple(i for run in runs for i in run)
    late = (HOPS - 2, HOPS - 1)
    known = []
    for run in runs[:-1]:
        known += head_mass(tables, q, lse, run, blocks(run))
    group = head_mass(tables, q, lse, runs[-1], blocks(runs[-1]), known, n_head)
    masses = [list(group)]
    masses.append(list(head_mass(tables, q, lse, late, blocks(late), (), n_head)))
    grads = {}
    for ids, mass in zip((early, late), masses):
        for turn in range(1, n_head):
            mass[turn] = around(mass[turn], turn)
        target = index_logits(tables, parts, weights, lse_share, ids, blocks(ids), latent)
        found = index_grad(tables, parts, weights, mass, target, ids, blocks(ids), latent)
        grads.update(zip(ids, found))

    total = grads[0] + lax.ppermute(grads[1], "seq", back)
    for m in range(1, HOPS // 2):
        both = grads[2 * m] + lax.ppermute(grads[2 * m + 1], "seq", swap)
        if m < HOPS // 2 - 1:
            total = total + lax.ppermute(both, "seq", ring(-2 * m))
    if n_head != 2:
        return lax.psum(total + lax.ppermute(both, "seq", ring(-2 * m)), "head")
    last = []
    for turn in range(2):
        route = [
            (2 * i + x, 2 * ((i - 2 * m) % n_seq) + (x + turn) % 2) for i in devices for x in range(2)
        ]
        last.append(lax.ppermute(both, ("seq", "head"), route))
    total = total + around(total, 1)
    return total + (last[0] + last[1])


def solution(mesh):
    placed = (
        P("seq", "head", None),
        P("seq", None),
        P("seq", "head"),
        P("seq", "head", None),
        P("seq", "head"),
        P("seq", None),
        P("seq"),
        P(),
        P(),
    )
    return jax.shard_map(
        body, mesh=mesh, in_specs=placed, out_specs=P("seq", None), check_vma=False
    )
```

```python
import functools
import math

import jax
import jax.numpy as jnp
from jax import lax
from jax.experimental import pallas as pl
from jax.experimental.pallas import tpu as pltpu
from jax.sharding import PartitionSpec as P


HEADS = 128
HOPS = 8
LOG2E = math.log2(math.e)
MAIN_SCALE = 1.0 / 192.0**0.5
LIMIT = 20 * 2**20
CUT_COST = 10**10
NT = (((1,), (1,)), ((), ()))
NN = (((1,), (0,)), ((), ()))
VMEM = pl.BlockSpec(memory_space=pltpu.VMEM)
SMEM = pl.BlockSpec(memory_space=pltpu.SMEM)
HBM = pl.BlockSpec(memory_space=pltpu.HBM)


def cut_kernel(block_ref, queries_ref, block_out, *rest):
    del block_ref, block_out
    shares, sems = rest[:-1], rest[-1]
    n, share = len(shares), shares[0].shape[0]
    copies = []
    for turn, out in enumerate(shares):
        start = lax.rem(lax.axis_index("head") + turn, n) * share
        part = queries_ref.at[pl.ds(start, share)]
        copies.append(pltpu.make_async_copy(part, out, sems.at[turn]))
    for copy in copies:
        copy.start()
    for copy in copies:
        copy.wait()


def cut_shares(block, index_queries, n_head):
    tokens, index_here, idx_width = index_queries.shape
    share = jax.ShapeDtypeStruct((tokens // n_head, index_here, idx_width), index_queries.dtype)
    block, *shares = pl.pallas_call(
        cut_kernel,
        in_specs=[VMEM, HBM],
        out_specs=[VMEM] * (1 + n_head),
        out_shape=[jax.ShapeDtypeStruct(block.shape, block.dtype)] + [share] * n_head,
        input_output_aliases={0: 0},
        scratch_shapes=[pltpu.SemaphoreType.DMA((n_head,))],
        cost_estimate=cost(CUT_COST),
        compiler_params=pltpu.CompilerParams(vmem_limit_bytes=LIMIT),
        name="cut_shares",
    )(block, index_queries)
    return block, shares


def facts(slot, order_ref, live_ref):
    n = lax.axis_size("seq")
    me = lax.axis_index("seq")
    crossed = (slot % 2 == 1) & (me % 2 == 0)
    hop = jnp.where(crossed, jnp.where(slot == 1, HOPS - 1, slot - 2), slot)
    own = order_ref[me]
    slab = order_ref[lax.rem(me - hop + n, n)]
    return slab - own, (slab <= own) & (live_ref[own, slab] == 1)


def packed(ids, order_ref, live_ref):
    count, slots = jnp.int32(0), []
    for i in ids:
        later, alive = facts(i, order_ref, live_ref)
        slots.append((count, later, alive))
        count = count + alive.astype(jnp.int32)
    return slots, count


def side_by_side(values):
    if len(values) % 2:
        values = values + [jnp.zeros_like(values[0])]
    pairs = [jnp.concatenate(values[i : i + 2], axis=1) for i in range(0, len(values), 2)]
    return jnp.concatenate(pairs, axis=0)


def side_by_side_shape(n, rows, share):
    return jax.ShapeDtypeStruct(((n + 1) // 2 * rows, 2 * share), jnp.float32)


def at(place, rows, blocks=1):
    return pl.ds(pl.multiple_of(place * rows, rows), blocks * rows)


def in_pairs(count, most, rows, work):
    def two(i, carry):
        work(at(2 * i, rows, 2))
        return carry

    if most == 2:
        pl.when(count == 2)(lambda: work(pl.ds(0, 2 * rows)))
    elif most > 2:
        lax.fori_loop(0, count // 2, two, 0)

    @pl.when(count % 2 == 1)
    def _():
        work(at(count - 1, rows))


def cost(flops):
    return pl.CostEstimate(flops=flops, transcendentals=0, bytes_accessed=flops // 256)


def score_kernel(ids, n_outs, pack, order_ref, live_ref, q_ref, lse_ref, *refs):
    blocks, known = refs[: len(ids)], refs[len(ids) : -n_outs - 2]
    outs, (keys, mass) = refs[-n_outs - 2 : -2], refs[-2:]
    heads, latent, tokens = q_ref.shape
    rows = blocks[0].shape[1]
    slots, count = packed(ids, order_ref, live_ref)
    for block, (place, _, alive) in zip(blocks, slots):

        @pl.when(alive)
        def _(block=block, place=place):
            keys[at(place, rows), :] = block[:latent, :].T

    def work(here):
        held = keys[here, :]
        total = None
        for h in range(0, heads, 2):
            pair = jnp.concatenate([q_ref[h], q_ref[h + 1]], axis=1)
            s = lax.dot_general(held, pair, NN, preferred_element_type=jnp.float32)
            s = s * (MAIN_SCALE * LOG2E)
            for n in range(2):
                lse = lse_ref[h + n : h + n + 1, :] * LOG2E
                p = jnp.exp2(s[:, n * tokens : (n + 1) * tokens] - lse)
                total = p if total is None else total + p
        mass[here, :] = total

    in_pairs(count, len(blocks), rows, work)
    values = [jnp.where(alive, mass[at(place, rows), :], 0.0) for place, _, alive in slots]
    if not pack:
        for out, value in zip(outs, values):
            out[...] = value
        return
    values = [ref[...] for ref in known] + values
    share = tokens // n_outs
    if n_outs > 1:
        turn = tokens - lax.axis_index("head") * share
        values = [pltpu.roll(value, turn, 1) for value in values]
    for n, out in enumerate(outs):
        out[...] = side_by_side([value[:, n * share : (n + 1) * share] for value in values])


def head_mass(tables, q, lse, ids, blocks, known=(), n_head=0):
    heads, latent, tokens = q.shape
    n, rows = len(ids), blocks[0].shape[1]
    shapes = [jax.ShapeDtypeStruct((rows, tokens), jnp.float32)] * n
    if n_head:
        shapes = [side_by_side_shape(n + len(known), rows, tokens // n_head)] * n_head
    return pl.pallas_call(
        functools.partial(score_kernel, ids, len(shapes), n_head > 0),
        in_specs=[SMEM, SMEM] + [VMEM] * (2 + n + len(known)),
        out_specs=[VMEM] * len(shapes),
        out_shape=shapes,
        scratch_shapes=[
            pltpu.VMEM((n * rows, latent), jnp.bfloat16),
            pltpu.VMEM((n * rows, tokens), jnp.float32),
        ],
        cost_estimate=cost(2 * tokens * heads * latent * n * rows),
        compiler_params=pltpu.CompilerParams(vmem_limit_bytes=LIMIT),
        name="score_mass",
    )(*tables, q, lse, *blocks, *known)


def lanes_of(part, share):
    return max(1, min(part.shape[0], 128 // share))


def pieces(part, share, width):
    side = lanes_of(part, share)
    step = part.shape[0] // side
    run = max(1, min(step, width))
    for first in range(0, step, run):
        heads = [part[k + n * step] for k in range(first, first + run) for n in range(side)]
        yield run, jnp.concatenate(heads, axis=0)


def lay_weights(parts, w_refs, w_lanes):
    row = 0
    for part, w_ref in zip(parts, w_refs):
        index_here, tokens = w_ref.shape
        share = part.shape[1]
        w = w_ref[...]
        if share < tokens:
            w = pltpu.roll(w, tokens - lax.axis_index("head") * share, 1)
        side = lanes_of(part, share)
        step = index_here // side
        tile = [w[n * step : (n + 1) * step, :share] for n in range(side)]
        w_lanes[row : row + step, :] = jnp.concatenate(tile, axis=1)
        row += step


def logit_kernel(latent, ids, n_head, order_ref, live_ref, *refs):
    parts, w_refs, lse_ref = refs[:n_head], refs[n_head : 2 * n_head], refs[2 * n_head]
    blocks, (out_ref, w_ref, keys, values) = refs[2 * n_head + 1 : -4], refs[-4:]
    rows, idx_width = blocks[0].shape[1], keys.shape[1]
    share = parts[0].shape[1]
    scale = 1.0 / idx_width**0.5
    lay_weights(parts, w_refs, w_ref)
    tile = w_ref.shape[1]
    lse = lse_ref[...]
    if share < lse.shape[1]:
        lse = pltpu.roll(lse, lse.shape[1] - lax.axis_index("head") * share, 1)[:, :share]
    slots, count = packed(ids, order_ref, live_ref)
    for block, (place, _, alive) in zip(blocks, slots):

        @pl.when(alive)
        def _(block=block, place=place):
            keys[at(place, rows), :] = block[latent:, :]

    def work(here):
        held = keys[here, :]
        acc = jnp.zeros((held.shape[0], tile), jnp.float32)
        row = 0
        for part in parts:
            for run, piece in pieces(part, share, 8):
                r = lax.dot_general(held, piece, NT, preferred_element_type=jnp.float32)
                for k in range(run):
                    relu = jnp.maximum(r[:, k * tile : (k + 1) * tile], 0.0)
                    acc = acc + relu * w_ref[row + k : row + k + 1, :]
                row += run
        logits = acc[:, :share]
        for first in range(share, tile, share):
            logits = logits + acc[:, first : first + share]
        values[here, :] = jnp.exp(logits * scale - lse)

    in_pairs(count, len(blocks), rows, work)
    out_ref[...] = side_by_side([jnp.where(s[2], values[at(s[0], rows), :], 0.0) for s in slots])


def index_logits(tables, parts, weights, lse, ids, blocks, latent):
    n_head, (index_here, share, idx_width) = len(parts), parts[0].shape
    rows = blocks[0].shape[1]
    side = lanes_of(parts[0], share)
    return pl.pallas_call(
        functools.partial(logit_kernel, latent, ids, n_head),
        in_specs=[SMEM, SMEM] + [VMEM] * (2 * n_head + 1 + len(blocks)),
        out_specs=VMEM,
        out_shape=side_by_side_shape(len(blocks), rows, share),
        scratch_shapes=[
            pltpu.VMEM((n_head * index_here // side, side * share), jnp.float32),
            pltpu.VMEM((len(blocks) * rows, idx_width), jnp.bfloat16),
            pltpu.VMEM((len(blocks) * rows, share), jnp.float32),
        ],
        cost_estimate=cost(2 * len(blocks) * rows * share * n_head * index_here * idx_width),
        compiler_params=pltpu.CompilerParams(vmem_limit_bytes=LIMIT),
        name="index_logits",
    )(*tables, *parts, *weights, lse, *blocks)


def grad_kernel(latent, ids, n_head, order_ref, live_ref, *refs):
    parts, w_refs, masses = refs[:n_head], refs[n_head : 2 * n_head], refs[2 * n_head : 3 * n_head]
    target_ref, (w_ref, keys, grads, results) = refs[3 * n_head], refs[-4:]
    n_blocks = (len(refs) - 3 * n_head - 5) // 2
    blocks, outs = refs[3 * n_head + 1 : -n_blocks - 4], refs[-n_blocks - 4 : -4]
    rows = blocks[0].shape[1]
    share, idx_width = parts[0].shape[1:]
    scale = 1.0 / idx_width**0.5
    lay_weights(parts, w_refs, w_ref)
    tile = w_ref.shape[1]
    start = lax.axis_index("head") * share
    slots, count = packed(ids, order_ref, live_ref)
    for i, (place, later, alive) in enumerate(slots):

        @pl.when(alive)
        def _(i=i, place=place, later=later):
            here = slice(i // 2 * rows, (i // 2 + 1) * rows)
            span = slice(i % 2 * share, (i % 2 + 1) * share)
            mass = masses[0][here, span]
            for other in masses[1:]:
                mass = mass + other[here, span]
            value = target_ref[here, span] - mass * (1.0 / HEADS)
            within = lax.broadcasted_iota(jnp.int32, (rows, share), 0)
            token = lax.broadcasted_iota(jnp.int32, (rows, share), 1) + start
            grad = jnp.where(within + later * rows <= token, value, 0.0)
            grads[at(place, rows), :] = jnp.concatenate([grad] * (tile // share), axis=1)
            keys[at(place, rows), :] = blocks[i][latent:, :]

    def work(here):
        held = keys[here, :]
        grad = grads[here, :]
        total = jnp.zeros((held.shape[0], idx_width), jnp.float32)
        row = 0
        for part in parts:
            for run, piece in pieces(part, share, 8):
                r = lax.dot_general(held, piece, NT, preferred_element_type=jnp.float32)
                weighted = []
                for k in range(run):
                    w = grad * w_ref[row + k : row + k + 1, :]
                    w = jnp.where(r[:, k * tile : (k + 1) * tile] > 0.0, w, 0.0)
                    weighted.append(w.astype(jnp.bfloat16))
                row += run
                total = total + lax.dot_general(
                    jnp.concatenate(weighted, axis=1), piece, NN, preferred_element_type=jnp.float32
                )
        results[here, :] = total * scale

    in_pairs(count, len(blocks), rows, work)
    for out, (place, _, alive) in zip(outs, slots):
        out[...] = jnp.where(alive, results[at(place, rows), :], 0.0)


def index_grad(tables, parts, weights, masses, target, ids, blocks, latent):
    n_head, (index_here, share, idx_width) = len(parts), parts[0].shape
    rows = blocks[0].shape[1]
    side = lanes_of(parts[0], share)
    return pl.pallas_call(
        functools.partial(grad_kernel, latent, ids, n_head),
        in_specs=[SMEM, SMEM] + [VMEM] * (3 * n_head + 1 + len(blocks)),
        out_specs=[VMEM] * len(blocks),
        out_shape=[jax.ShapeDtypeStruct((rows, idx_width), jnp.float32)] * len(blocks),
        scratch_shapes=[
            pltpu.VMEM((n_head * index_here // side, side * share), jnp.float32),
            pltpu.VMEM((len(blocks) * rows, idx_width), jnp.bfloat16),
            pltpu.VMEM((len(blocks) * rows, side * share), jnp.float32),
            pltpu.VMEM((len(blocks) * rows, idx_width), jnp.float32),
        ],
        cost_estimate=cost(4 * len(blocks) * rows * share * n_head * index_here * idx_width),
        compiler_params=pltpu.CompilerParams(vmem_limit_bytes=LIMIT),
        name="index_grad",
    )(*tables, *parts, *weights, *masses, target, *blocks)


def body(
    q_main,
    latent_keys,
    lse_main,
    index_queries,
    index_weights,
    index_keys,
    lse_index,
    slab_order,
    block_live,
):
    n_seq = lax.axis_size("seq")
    n_head = lax.axis_size("head")
    latent = latent_keys.shape[1]
    devices = range(n_seq)

    def ring(distance):
        return [(i, (i + distance) % n_seq) for i in devices]

    def around(array, turn):
        return lax.ppermute(array, "head", [(i, (i + turn) % n_head) for i in range(n_head)])

    forward = [(i, (i + (HOPS - 1 if i % 2 else 1)) % n_seq) for i in devices]
    back = [(b, a) for a, b in forward]
    swap = [(i, i ^ 1) for i in devices]
    own = jnp.concatenate([latent_keys.T, index_keys], axis=0)
    own, shares = cut_shares(own, index_queries, n_head)
    arrived = [lax.ppermute(own, "seq", ring(2))]
    arrived.append(lax.ppermute(own, "seq", ring(4)))
    slots = [own, lax.ppermute(own, "seq", forward)]
    for m in range(1, HOPS // 2):
        if m > 2:
            arrived.append(lax.ppermute(arrived[m - 3], "seq", ring(4)))
        slots += [arrived[m - 1], lax.ppermute(arrived[m - 1], "seq", swap)]

    turns = range(n_head)
    weights = [around(index_weights.T, turn) if turn else index_weights.T for turn in turns]
    parts = [around(shares[turn], turn) if turn else shares[turn] for turn in turns]
    parts = [part.transpose(1, 0, 2) for part in parts]

    tables = slab_order, block_live
    q, lse, lse_share = q_main.transpose(1, 2, 0), lse_main.T, lse_index[None, :]

    def blocks(ids):
        return [slots[i] for i in ids]

    runs = [(0,)] + [(2 * m, 2 * m + 1) for m in range(1, HOPS // 2 - 1)]
    runs[-1] += (1,)
    early = tuple(i for run in runs for i in run)
    late = (HOPS - 2, HOPS - 1)
    known = []
    for run in runs[:-1]:
        known += head_mass(tables, q, lse, run, blocks(run))
    group = head_mass(tables, q, lse, runs[-1], blocks(runs[-1]), known, n_head)
    masses = [list(group)]
    masses.append(list(head_mass(tables, q, lse, late, blocks(late), (), n_head)))
    grads = {}
    for ids, mass in zip((early, late), masses):
        for turn in range(1, n_head):
            mass[turn] = around(mass[turn], turn)
        target = index_logits(tables, parts, weights, lse_share, ids, blocks(ids), latent)
        found = index_grad(tables, parts, weights, mass, target, ids, blocks(ids), latent)
        grads.update(zip(ids, found))

    total = grads[0] + lax.ppermute(grads[1], "seq", back)
    for m in range(1, HOPS // 2):
        both = grads[2 * m] + lax.ppermute(grads[2 * m + 1], "seq", swap)
        if m < HOPS // 2 - 1:
            total = total + lax.ppermute(both, "seq", ring(-2 * m))
    if n_head != 2:
        return lax.psum(total + lax.ppermute(both, "seq", ring(-2 * m)), "head")
    last = []
    for turn in range(2):
        route = [
            (2 * i + x, 2 * ((i - 2 * m) % n_seq) + (x + turn) % 2) for i in devices for x in range(2)
        ]
        last.append(lax.ppermute(both.astype(jnp.bfloat16), ("seq", "head"), route))
    total = total + around(total, 1)
    return total + (last[0].astype(jnp.float32) + last[1].astype(jnp.float32))


def solution(mesh):
    placed = (
        P("seq", "head", None),
        P("seq", None),
        P("seq", "head"),
        P("seq", "head", None),
        P("seq", "head"),
        P("seq", None),
        P("seq"),
        P(),
        P(),
    )
    return jax.shard_map(
        body, mesh=mesh, in_specs=placed, out_specs=P("seq", None), check_vma=False
    )
```

```python
import functools
import math

import jax
import jax.numpy as jnp
from jax import lax
from jax.experimental import pallas as pl
from jax.experimental.pallas import tpu as pltpu
from jax.sharding import PartitionSpec as P


HEADS = 128
HOPS = 8
LOG2E = math.log2(math.e)
MAIN_SCALE = 1.0 / 192.0**0.5
LIMIT = 20 * 2**20
CUT_COST = 10**10
NT = (((1,), (1,)), ((), ()))
NN = (((1,), (0,)), ((), ()))
VMEM = pl.BlockSpec(memory_space=pltpu.VMEM)
SMEM = pl.BlockSpec(memory_space=pltpu.SMEM)
HBM = pl.BlockSpec(memory_space=pltpu.HBM)


def cut_kernel(block_ref, queries_ref, block_out, *rest):
    del block_ref, block_out
    shares, sems = rest[:-1], rest[-1]
    n, share = len(shares), shares[0].shape[0]
    copies = []
    for turn, out in enumerate(shares):
        start = lax.rem(lax.axis_index("head") + turn, n) * share
        part = queries_ref.at[pl.ds(start, share)]
        copies.append(pltpu.make_async_copy(part, out, sems.at[turn]))
    for copy in copies:
        copy.start()
    for copy in copies:
        copy.wait()


def cut_shares(block, index_queries, n_head):
    tokens, index_here, idx_width = index_queries.shape
    share = jax.ShapeDtypeStruct((tokens // n_head, index_here, idx_width), index_queries.dtype)
    block, *shares = pl.pallas_call(
        cut_kernel,
        in_specs=[VMEM, HBM],
        out_specs=[VMEM] * (1 + n_head),
        out_shape=[jax.ShapeDtypeStruct(block.shape, block.dtype)] + [share] * n_head,
        input_output_aliases={0: 0},
        scratch_shapes=[pltpu.SemaphoreType.DMA((n_head,))],
        cost_estimate=cost(CUT_COST),
        compiler_params=pltpu.CompilerParams(vmem_limit_bytes=LIMIT),
        name="cut_shares",
    )(block, index_queries)
    return block, shares


def facts(slot, order_ref, live_ref):
    n = lax.axis_size("seq")
    me = lax.axis_index("seq")
    crossed = (slot % 2 == 1) & (me % 2 == 0)
    hop = jnp.where(crossed, jnp.where(slot == 1, HOPS - 1, slot - 2), slot)
    own = order_ref[me]
    slab = order_ref[lax.rem(me - hop + n, n)]
    return slab - own, (slab <= own) & (live_ref[own, slab] == 1)


def packed(ids, facts_ref):
    count, slots = jnp.int32(0), []
    for i in ids:
        alive = facts_ref[2 * i + 1]
        slots.append((count, facts_ref[2 * i], alive == 1))
        count = count + alive
    return slots, count


def side_by_side(values):
    if len(values) % 2:
        values = values + [jnp.zeros_like(values[0])]
    pairs = [jnp.concatenate(values[i : i + 2], axis=1) for i in range(0, len(values), 2)]
    return jnp.concatenate(pairs, axis=0)


def side_by_side_shape(n, rows, share):
    return jax.ShapeDtypeStruct(((n + 1) // 2 * rows, 2 * share), jnp.float32)


def at(place, rows, blocks=1):
    return pl.ds(pl.multiple_of(place * rows, rows), blocks * rows)


def in_pairs(count, most, rows, work):
    def two(i, carry):
        work(at(2 * i, rows, 2))
        return carry

    if most == 2:
        pl.when(count == 2)(lambda: work(pl.ds(0, 2 * rows)))
    elif most > 2:
        lax.fori_loop(0, count // 2, two, 0)

    @pl.when(count % 2 == 1)
    def _():
        work(at(count - 1, rows))


def cost(flops):
    return pl.CostEstimate(flops=flops, transcendentals=0, bytes_accessed=flops // 256)


def score_kernel(ids, n_outs, pack, facts_ref, q_ref, lse_ref, *refs):
    blocks, known = refs[: len(ids)], refs[len(ids) : -n_outs - 2]
    outs, (keys, mass) = refs[-n_outs - 2 : -2], refs[-2:]
    heads, latent, tokens = q_ref.shape
    rows = blocks[0].shape[1]
    slots, count = packed(ids, facts_ref)
    for block, (place, _, alive) in zip(blocks, slots):

        @pl.when(alive)
        def _(block=block, place=place):
            keys[at(place, rows), :] = block[:latent, :].T

    def work(here):
        held = keys[here, :]
        total = None
        for h in range(0, heads, 2):
            pair = jnp.concatenate([q_ref[h], q_ref[h + 1]], axis=1)
            s = lax.dot_general(held, pair, NN, preferred_element_type=jnp.float32)
            s = s * (MAIN_SCALE * LOG2E)
            for n in range(2):
                lse = lse_ref[h + n : h + n + 1, :] * LOG2E
                p = jnp.exp2(s[:, n * tokens : (n + 1) * tokens] - lse)
                total = p if total is None else total + p
        mass[here, :] = total

    in_pairs(count, len(blocks), rows, work)
    values = [jnp.where(alive, mass[at(place, rows), :], 0.0) for place, _, alive in slots]
    if not pack:
        for out, value in zip(outs, values):
            out[...] = value
        return
    values = [ref[...] for ref in known] + values
    share = tokens // n_outs
    if n_outs > 1:
        turn = tokens - lax.axis_index("head") * share
        values = [pltpu.roll(value, turn, 1) for value in values]
    for n, out in enumerate(outs):
        out[...] = side_by_side([value[:, n * share : (n + 1) * share] for value in values])


def head_mass(known_facts, q, lse, ids, blocks, known=(), n_head=0):
    heads, latent, tokens = q.shape
    n, rows = len(ids), blocks[0].shape[1]
    shapes = [jax.ShapeDtypeStruct((rows, tokens), jnp.float32)] * n
    if n_head:
        shapes = [side_by_side_shape(n + len(known), rows, tokens // n_head)] * n_head
    return pl.pallas_call(
        functools.partial(score_kernel, ids, len(shapes), n_head > 0),
        in_specs=[SMEM] + [VMEM] * (2 + n + len(known)),
        out_specs=[VMEM] * len(shapes),
        out_shape=shapes,
        scratch_shapes=[
            pltpu.VMEM((n * rows, latent), jnp.bfloat16),
            pltpu.VMEM((n * rows, tokens), jnp.float32),
        ],
        cost_estimate=cost(2 * tokens * heads * latent * n * rows),
        compiler_params=pltpu.CompilerParams(vmem_limit_bytes=LIMIT),
        name="score_mass",
    )(known_facts, q, lse, *blocks, *known)


def first_kernel(order_ref, live_ref, q_ref, lse_ref, block_ref, facts_ref, mass_ref, keys, mass):
    for i in range(HOPS):
        later, alive = facts(i, order_ref, live_ref)
        facts_ref[2 * i] = later
        facts_ref[2 * i + 1] = alive.astype(jnp.int32)
    score_kernel((0,), 1, False, facts_ref, q_ref, lse_ref, block_ref, mass_ref, keys, mass)


def first_mass(order, live, q, lse, block):
    heads, latent, tokens = q.shape
    rows = block.shape[1]
    return pl.pallas_call(
        first_kernel,
        in_specs=[SMEM, SMEM] + [VMEM] * 3,
        out_specs=[SMEM, VMEM],
        out_shape=[
            jax.ShapeDtypeStruct((2 * HOPS,), jnp.int32),
            jax.ShapeDtypeStruct((rows, tokens), jnp.float32),
        ],
        scratch_shapes=[
            pltpu.VMEM((rows, latent), jnp.bfloat16),
            pltpu.VMEM((rows, tokens), jnp.float32),
        ],
        cost_estimate=cost(2 * tokens * heads * latent * rows),
        compiler_params=pltpu.CompilerParams(vmem_limit_bytes=LIMIT),
        name="first_mass",
    )(order, live, q, lse, block)


def lanes_of(part, share):
    return max(1, min(part.shape[0], 128 // share))


def pieces(part, share, width):
    side = lanes_of(part, share)
    step = part.shape[0] // side
    run = max(1, min(step, width))
    for first in range(0, step, run):
        heads = [part[k + n * step] for k in range(first, first + run) for n in range(side)]
        yield run, jnp.concatenate(heads, axis=0)


def lay_weights(parts, w_refs, w_lanes):
    row = 0
    for part, w_ref in zip(parts, w_refs):
        index_here, tokens = w_ref.shape
        share = part.shape[1]
        w = w_ref[...]
        if share < tokens:
            w = pltpu.roll(w, tokens - lax.axis_index("head") * share, 1)
        side = lanes_of(part, share)
        step = index_here // side
        tile = [w[n * step : (n + 1) * step, :share] for n in range(side)]
        w_lanes[row : row + step, :] = jnp.concatenate(tile, axis=1)
        row += step


def logit_kernel(latent, ids, n_head, facts_ref, *refs):
    parts, w_refs, lse_ref = refs[:n_head], refs[n_head : 2 * n_head], refs[2 * n_head]
    blocks, (out_ref, w_ref, keys, values) = refs[2 * n_head + 1 : -4], refs[-4:]
    rows, idx_width = blocks[0].shape[1], keys.shape[1]
    share = parts[0].shape[1]
    scale = 1.0 / idx_width**0.5
    lay_weights(parts, w_refs, w_ref)
    tile = w_ref.shape[1]
    lse = lse_ref[...]
    if share < lse.shape[1]:
        lse = pltpu.roll(lse, lse.shape[1] - lax.axis_index("head") * share, 1)[:, :share]
    slots, count = packed(ids, facts_ref)
    for block, (place, _, alive) in zip(blocks, slots):

        @pl.when(alive)
        def _(block=block, place=place):
            keys[at(place, rows), :] = block[latent:, :]

    def work(here):
        held = keys[here, :]
        acc = jnp.zeros((held.shape[0], tile), jnp.float32)
        row = 0
        for part in parts:
            for run, piece in pieces(part, share, 8):
                r = lax.dot_general(held, piece, NT, preferred_element_type=jnp.float32)
                for k in range(run):
                    relu = jnp.maximum(r[:, k * tile : (k + 1) * tile], 0.0)
                    acc = acc + relu * w_ref[row + k : row + k + 1, :]
                row += run
        logits = acc[:, :share]
        for first in range(share, tile, share):
            logits = logits + acc[:, first : first + share]
        values[here, :] = jnp.exp(logits * scale - lse)

    in_pairs(count, len(blocks), rows, work)
    out_ref[...] = side_by_side([jnp.where(s[2], values[at(s[0], rows), :], 0.0) for s in slots])


def index_logits(known_facts, parts, weights, lse, ids, blocks, latent):
    n_head, (index_here, share, idx_width) = len(parts), parts[0].shape
    rows = blocks[0].shape[1]
    side = lanes_of(parts[0], share)
    return pl.pallas_call(
        functools.partial(logit_kernel, latent, ids, n_head),
        in_specs=[SMEM] + [VMEM] * (2 * n_head + 1 + len(blocks)),
        out_specs=VMEM,
        out_shape=side_by_side_shape(len(blocks), rows, share),
        scratch_shapes=[
            pltpu.VMEM((n_head * index_here // side, side * share), jnp.float32),
            pltpu.VMEM((len(blocks) * rows, idx_width), jnp.bfloat16),
            pltpu.VMEM((len(blocks) * rows, share), jnp.float32),
        ],
        cost_estimate=cost(2 * len(blocks) * rows * share * n_head * index_here * idx_width),
        compiler_params=pltpu.CompilerParams(vmem_limit_bytes=LIMIT),
        name="index_logits",
    )(known_facts, *parts, *weights, lse, *blocks)


def grad_kernel(latent, ids, n_head, facts_ref, *refs):
    parts, w_refs, masses = refs[:n_head], refs[n_head : 2 * n_head], refs[2 * n_head : 3 * n_head]
    target_ref, (w_ref, keys, grads, results) = refs[3 * n_head], refs[-4:]
    n_blocks = (len(refs) - 3 * n_head - 5) // 2
    blocks, outs = refs[3 * n_head + 1 : -n_blocks - 4], refs[-n_blocks - 4 : -4]
    rows = blocks[0].shape[1]
    share, idx_width = parts[0].shape[1:]
    scale = 1.0 / idx_width**0.5
    lay_weights(parts, w_refs, w_ref)
    tile = w_ref.shape[1]
    start = lax.axis_index("head") * share
    slots, count = packed(ids, facts_ref)
    for i, (place, later, alive) in enumerate(slots):

        @pl.when(alive)
        def _(i=i, place=place, later=later):
            here = slice(i // 2 * rows, (i // 2 + 1) * rows)
            span = slice(i % 2 * share, (i % 2 + 1) * share)
            mass = masses[0][here, span]
            for other in masses[1:]:
                mass = mass + other[here, span]
            value = target_ref[here, span] - mass * (1.0 / HEADS)
            within = lax.broadcasted_iota(jnp.int32, (rows, share), 0)
            token = lax.broadcasted_iota(jnp.int32, (rows, share), 1) + start
            grad = jnp.where(within + later * rows <= token, value, 0.0)
            grads[at(place, rows), :] = jnp.concatenate([grad] * (tile // share), axis=1)
            keys[at(place, rows), :] = blocks[i][latent:, :]

    def work(here):
        held = keys[here, :]
        grad = grads[here, :]
        total = jnp.zeros((held.shape[0], idx_width), jnp.float32)
        row = 0
        for part in parts:
            for run, piece in pieces(part, share, 8):
                r = lax.dot_general(held, piece, NT, preferred_element_type=jnp.float32)
                weighted = []
                for k in range(run):
                    w = grad * w_ref[row + k : row + k + 1, :]
                    w = jnp.where(r[:, k * tile : (k + 1) * tile] > 0.0, w, 0.0)
                    weighted.append(w.astype(jnp.bfloat16))
                row += run
                total = total + lax.dot_general(
                    jnp.concatenate(weighted, axis=1), piece, NN, preferred_element_type=jnp.float32
                )
        results[here, :] = total * scale

    in_pairs(count, len(blocks), rows, work)
    for out, (place, _, alive) in zip(outs, slots):
        out[...] = jnp.where(alive, results[at(place, rows), :], 0.0)


def index_grad(known_facts, parts, weights, masses, target, ids, blocks, latent):
    n_head, (index_here, share, idx_width) = len(parts), parts[0].shape
    rows = blocks[0].shape[1]
    side = lanes_of(parts[0], share)
    return pl.pallas_call(
        functools.partial(grad_kernel, latent, ids, n_head),
        in_specs=[SMEM] + [VMEM] * (3 * n_head + 1 + len(blocks)),
        out_specs=[VMEM] * len(blocks),
        out_shape=[jax.ShapeDtypeStruct((rows, idx_width), jnp.float32)] * len(blocks),
        scratch_shapes=[
            pltpu.VMEM((n_head * index_here // side, side * share), jnp.float32),
            pltpu.VMEM((len(blocks) * rows, idx_width), jnp.bfloat16),
            pltpu.VMEM((len(blocks) * rows, side * share), jnp.float32),
            pltpu.VMEM((len(blocks) * rows, idx_width), jnp.float32),
        ],
        cost_estimate=cost(4 * len(blocks) * rows * share * n_head * index_here * idx_width),
        compiler_params=pltpu.CompilerParams(vmem_limit_bytes=LIMIT),
        name="index_grad",
    )(known_facts, *parts, *weights, *masses, target, *blocks)


def body(
    q_main,
    latent_keys,
    lse_main,
    index_queries,
    index_weights,
    index_keys,
    lse_index,
    slab_order,
    block_live,
):
    n_seq = lax.axis_size("seq")
    n_head = lax.axis_size("head")
    latent = latent_keys.shape[1]
    devices = range(n_seq)

    def ring(distance):
        return [(i, (i + distance) % n_seq) for i in devices]

    def around(array, turn):
        return lax.ppermute(array, "head", [(i, (i + turn) % n_head) for i in range(n_head)])

    forward = [(i, (i + (HOPS - 1 if i % 2 else 1)) % n_seq) for i in devices]
    back = [(b, a) for a, b in forward]
    swap = [(i, i ^ 1) for i in devices]
    own = jnp.concatenate([latent_keys.T, index_keys], axis=0)
    own, shares = cut_shares(own, index_queries, n_head)
    arrived = [lax.ppermute(own, "seq", ring(2))]
    arrived.append(lax.ppermute(own, "seq", ring(4)))
    slots = [own, lax.ppermute(own, "seq", forward)]
    for m in range(1, HOPS // 2):
        if m > 2:
            arrived.append(lax.ppermute(arrived[m - 3], "seq", ring(4)))
        slots += [arrived[m - 1], lax.ppermute(arrived[m - 1], "seq", swap)]

    turns = range(n_head)
    weights = [around(index_weights.T, turn) if turn else index_weights.T for turn in turns]
    parts = [around(shares[turn], turn) if turn else shares[turn] for turn in turns]
    parts = [part.transpose(1, 0, 2) for part in parts]

    q, lse, lse_share = q_main.transpose(1, 2, 0), lse_main.T, lse_index[None, :]

    def blocks(ids):
        return [slots[i] for i in ids]

    runs = [(0,)] + [(2 * m, 2 * m + 1) for m in range(1, HOPS // 2 - 1)]
    runs[-1] += (1,)
    early = tuple(i for run in runs for i in run)
    late = (HOPS - 2, HOPS - 1)
    tables, own_mass = first_mass(slab_order, block_live, q, lse, own)
    known = [own_mass]
    for run in runs[1:-1]:
        known += head_mass(tables, q, lse, run, blocks(run))
    group = head_mass(tables, q, lse, runs[-1], blocks(runs[-1]), known, n_head)
    masses = [list(group)]
    masses.append(list(head_mass(tables, q, lse, late, blocks(late), (), n_head)))
    grads = {}
    for ids, mass in zip((early, late), masses):
        for turn in range(1, n_head):
            mass[turn] = around(mass[turn], turn)
        target = index_logits(tables, parts, weights, lse_share, ids, blocks(ids), latent)
        found = index_grad(tables, parts, weights, mass, target, ids, blocks(ids), latent)
        grads.update(zip(ids, found))

    total = grads[0] + lax.ppermute(grads[1], "seq", back)
    for m in range(1, HOPS // 2):
        both = grads[2 * m] + lax.ppermute(grads[2 * m + 1], "seq", swap)
        if m < HOPS // 2 - 1:
            total = total + lax.ppermute(both, "seq", ring(-2 * m))
    if n_head != 2:
        return lax.psum(total + lax.ppermute(both, "seq", ring(-2 * m)), "head")
    last = []
    for turn in range(2):
        route = [
            (2 * i + x, 2 * ((i - 2 * m) % n_seq) + (x + turn) % 2) for i in devices for x in range(2)
        ]
        last.append(lax.ppermute(both.astype(jnp.bfloat16), ("seq", "head"), route))
    total = total + around(total, 1)
    return total + (last[0].astype(jnp.float32) + last[1].astype(jnp.float32))


def solution(mesh):
    placed = (
        P("seq", "head", None),
        P("seq", None),
        P("seq", "head"),
        P("seq", "head", None),
        P("seq", "head"),
        P("seq", None),
        P("seq"),
        P(),
        P(),
    )
    return jax.shard_map(
        body, mesh=mesh, in_specs=placed, out_specs=P("seq", None), check_vma=False
    )
```

```python
import functools
import math

import jax
import jax.numpy as jnp
from jax import lax
from jax.experimental import pallas as pl
from jax.experimental.pallas import tpu as pltpu
from jax.sharding import PartitionSpec as P


HEADS = 128
HOPS = 8
LOG2E = math.log2(math.e)
MAIN_SCALE = 1.0 / 192.0**0.5
LIMIT = 20 * 2**20
CUT_COST = 10**10
NT = (((1,), (1,)), ((), ()))
NN = (((1,), (0,)), ((), ()))
VMEM = pl.BlockSpec(memory_space=pltpu.VMEM)
SMEM = pl.BlockSpec(memory_space=pltpu.SMEM)
HBM = pl.BlockSpec(memory_space=pltpu.HBM)


def cut_kernel(block_ref, queries_ref, block_out, *rest):
    del block_ref, block_out
    shares, sems = rest[:-1], rest[-1]
    n, share = len(shares), shares[0].shape[0]
    copies = []
    for turn, out in enumerate(shares):
        start = lax.rem(lax.axis_index("head") + turn, n) * share
        part = queries_ref.at[pl.ds(start, share)]
        copies.append(pltpu.make_async_copy(part, out, sems.at[turn]))
    for copy in copies:
        copy.start()
    for copy in copies:
        copy.wait()


def cut_shares(block, index_queries, n_head):
    tokens, index_here, idx_width = index_queries.shape
    share = jax.ShapeDtypeStruct((tokens // n_head, index_here, idx_width), index_queries.dtype)
    block, *shares = pl.pallas_call(
        cut_kernel,
        in_specs=[VMEM, HBM],
        out_specs=[VMEM] * (1 + n_head),
        out_shape=[jax.ShapeDtypeStruct(block.shape, block.dtype)] + [share] * n_head,
        input_output_aliases={0: 0},
        scratch_shapes=[pltpu.SemaphoreType.DMA((n_head,))],
        cost_estimate=cost(CUT_COST),
        compiler_params=pltpu.CompilerParams(vmem_limit_bytes=LIMIT),
        name="cut_shares",
    )(block, index_queries)
    return block, shares


def facts(slot, order_ref, live_ref):
    n = lax.axis_size("seq")
    me = lax.axis_index("seq")
    crossed = (slot % 2 == 1) & (me % 2 == 0)
    hop = jnp.where(crossed, jnp.where(slot == 1, HOPS - 1, slot - 2), slot)
    own = order_ref[me]
    slab = order_ref[lax.rem(me - hop + n, n)]
    return slab - own, (slab <= own) & (live_ref[own, slab] == 1)


def packed(ids, facts_ref):
    count, slots = jnp.int32(0), []
    for i in ids:
        alive = facts_ref[2 * i + 1]
        slots.append((count, facts_ref[2 * i], alive == 1))
        count = count + alive
    return slots, count


def side_by_side(values):
    if len(values) % 2:
        values = values + [jnp.zeros_like(values[0])]
    pairs = [jnp.concatenate(values[i : i + 2], axis=1) for i in range(0, len(values), 2)]
    return jnp.concatenate(pairs, axis=0)


def side_by_side_shape(n, rows, share):
    return jax.ShapeDtypeStruct(((n + 1) // 2 * rows, 2 * share), jnp.float32)


def at(place, rows, blocks=1):
    return pl.ds(pl.multiple_of(place * rows, rows), blocks * rows)


def in_pairs(count, most, rows, work):
    def two(i, carry):
        work(at(2 * i, rows, 2))
        return carry

    if most == 2:
        pl.when(count == 2)(lambda: work(pl.ds(0, 2 * rows)))
    elif most > 2:
        lax.fori_loop(0, count // 2, two, 0)

    @pl.when(count % 2 == 1)
    def _():
        work(at(count - 1, rows))


def cost(flops):
    return pl.CostEstimate(flops=flops, transcendentals=0, bytes_accessed=flops // 256)


def score_kernel(ids, n_outs, pack, facts_ref, q_ref, lse_ref, *refs):
    blocks, known = refs[: len(ids)], refs[len(ids) : -n_outs - 2]
    outs, (keys, mass) = refs[-n_outs - 2 : -2], refs[-2:]
    heads, latent, tokens = q_ref.shape
    rows = blocks[0].shape[1]
    slots, count = packed(ids, facts_ref)
    for block, (place, _, alive) in zip(blocks, slots):

        @pl.when(alive)
        def _(block=block, place=place):
            keys[at(place, rows), :] = block[:latent, :].T

    def work(here):
        held = keys[here, :]
        total = None
        for h in range(0, heads, 2):
            pair = jnp.concatenate([q_ref[h], q_ref[h + 1]], axis=1)
            s = lax.dot_general(held, pair, NN, preferred_element_type=jnp.float32)
            s = s * (MAIN_SCALE * LOG2E)
            for n in range(2):
                lse = lse_ref[h + n : h + n + 1, :] * LOG2E
                p = jnp.exp2(s[:, n * tokens : (n + 1) * tokens] - lse)
                total = p if total is None else total + p
        mass[here, :] = total

    in_pairs(count, len(blocks), rows, work)
    values = [jnp.where(alive, mass[at(place, rows), :], 0.0) for place, _, alive in slots]
    if not pack:
        for out, value in zip(outs, values):
            out[...] = value
        return
    values = [ref[...] for ref in known] + values
    share = tokens // n_outs
    if n_outs > 1:
        turn = tokens - lax.axis_index("head") * share
        values = [pltpu.roll(value, turn, 1) for value in values]
    for n, out in enumerate(outs):
        out[...] = side_by_side([value[:, n * share : (n + 1) * share] for value in values])


def head_mass(known_facts, q, lse, ids, blocks, known=(), n_head=0):
    heads, latent, tokens = q.shape
    n, rows = len(ids), blocks[0].shape[1]
    shapes = [jax.ShapeDtypeStruct((rows, tokens), jnp.float32)] * n
    if n_head:
        shapes = [side_by_side_shape(n + len(known), rows, tokens // n_head)] * n_head
    return pl.pallas_call(
        functools.partial(score_kernel, ids, len(shapes), n_head > 0),
        in_specs=[SMEM] + [VMEM] * (2 + n + len(known)),
        out_specs=[VMEM] * len(shapes),
        out_shape=shapes,
        scratch_shapes=[
            pltpu.VMEM((n * rows, latent), jnp.bfloat16),
            pltpu.VMEM((n * rows, tokens), jnp.float32),
        ],
        cost_estimate=cost(2 * tokens * heads * latent * n * rows),
        compiler_params=pltpu.CompilerParams(vmem_limit_bytes=LIMIT),
        name="score_mass",
    )(known_facts, q, lse, *blocks, *known)


def first_kernel(order_ref, live_ref, q_ref, lse_ref, block_ref, facts_ref, mass_ref, keys, mass):
    for i in range(HOPS):
        later, alive = facts(i, order_ref, live_ref)
        facts_ref[2 * i] = later
        facts_ref[2 * i + 1] = alive.astype(jnp.int32)
    score_kernel((0,), 1, False, facts_ref, q_ref, lse_ref, block_ref, mass_ref, keys, mass)


def first_mass(order, live, q, lse, block):
    heads, latent, tokens = q.shape
    rows = block.shape[1]
    return pl.pallas_call(
        first_kernel,
        in_specs=[SMEM, SMEM] + [VMEM] * 3,
        out_specs=[SMEM, VMEM],
        out_shape=[
            jax.ShapeDtypeStruct((2 * HOPS,), jnp.int32),
            jax.ShapeDtypeStruct((rows, tokens), jnp.float32),
        ],
        scratch_shapes=[
            pltpu.VMEM((rows, latent), jnp.bfloat16),
            pltpu.VMEM((rows, tokens), jnp.float32),
        ],
        cost_estimate=cost(2 * tokens * heads * latent * rows),
        compiler_params=pltpu.CompilerParams(vmem_limit_bytes=LIMIT),
        name="first_mass",
    )(order, live, q, lse, block)


def lanes_of(part, share):
    return max(1, min(part.shape[0], 128 // share))


def pieces(part, share, width):
    side = lanes_of(part, share)
    step = part.shape[0] // side
    run = max(1, min(step, width))
    for first in range(0, step, run):
        heads = [part[k + n * step] for k in range(first, first + run) for n in range(side)]
        yield run, jnp.concatenate(heads, axis=0)


def lay_weights(parts, w_refs, w_lanes):
    row = 0
    for part, w_ref in zip(parts, w_refs):
        index_here, tokens = w_ref.shape
        share = part.shape[1]
        w = w_ref[...]
        if share < tokens:
            w = pltpu.roll(w, tokens - lax.axis_index("head") * share, 1)
        side = lanes_of(part, share)
        step = index_here // side
        tile = [w[n * step : (n + 1) * step, :share] for n in range(side)]
        w_lanes[row : row + step, :] = jnp.concatenate(tile, axis=1)
        row += step


def logit_kernel(latent, ids, n_head, facts_ref, *refs):
    parts, w_refs, lse_ref = refs[:n_head], refs[n_head : 2 * n_head], refs[2 * n_head]
    blocks, (out_ref, relu_ref, w_ref, keys, values) = refs[2 * n_head + 1 : -5], refs[-5:]
    rows, idx_width = blocks[0].shape[1], keys.shape[1]
    share = parts[0].shape[1]
    scale = 1.0 / idx_width**0.5
    lay_weights(parts, w_refs, w_ref)
    tile = w_ref.shape[1]
    lse = lse_ref[...]
    if share < lse.shape[1]:
        lse = pltpu.roll(lse, lse.shape[1] - lax.axis_index("head") * share, 1)[:, :share]
    slots, count = packed(ids, facts_ref)
    for block, (place, _, alive) in zip(blocks, slots):

        @pl.when(alive)
        def _(block=block, place=place):
            keys[at(place, rows), :] = block[latent:, :]

    def work(here):
        held = keys[here, :]
        acc = jnp.zeros((held.shape[0], tile), jnp.float32)
        row = 0
        for part in parts:
            for run, piece in pieces(part, share, 8):
                r = lax.dot_general(held, piece, NT, preferred_element_type=jnp.float32)
                relu_ref[here, row * tile : (row + run) * tile] = r.astype(jnp.bfloat16)
                for k in range(run):
                    relu = jnp.maximum(r[:, k * tile : (k + 1) * tile], 0.0)
                    acc = acc + relu * w_ref[row + k : row + k + 1, :]
                row += run
        logits = acc[:, :share]
        for first in range(share, tile, share):
            logits = logits + acc[:, first : first + share]
        values[here, :] = jnp.exp(logits * scale - lse)

    in_pairs(count, len(blocks), rows, work)
    out_ref[...] = side_by_side([jnp.where(s[2], values[at(s[0], rows), :], 0.0) for s in slots])


def index_logits(known_facts, parts, weights, lse, ids, blocks, latent):
    n_head, (index_here, share, idx_width) = len(parts), parts[0].shape
    rows = blocks[0].shape[1]
    side = lanes_of(parts[0], share)
    return pl.pallas_call(
        functools.partial(logit_kernel, latent, ids, n_head),
        in_specs=[SMEM] + [VMEM] * (2 * n_head + 1 + len(blocks)),
        out_specs=[VMEM, VMEM],
        out_shape=[
            side_by_side_shape(len(blocks), rows, share),
            jax.ShapeDtypeStruct((len(blocks) * rows, n_head * index_here * share), jnp.bfloat16),
        ],
        scratch_shapes=[
            pltpu.VMEM((n_head * index_here // side, side * share), jnp.float32),
            pltpu.VMEM((len(blocks) * rows, idx_width), jnp.bfloat16),
            pltpu.VMEM((len(blocks) * rows, share), jnp.float32),
        ],
        cost_estimate=cost(2 * len(blocks) * rows * share * n_head * index_here * idx_width),
        compiler_params=pltpu.CompilerParams(vmem_limit_bytes=LIMIT),
        name="index_logits",
    )(known_facts, *parts, *weights, lse, *blocks)


def grad_kernel(ids, n_head, facts_ref, *refs):
    parts, w_refs, masses = refs[:n_head], refs[n_head : 2 * n_head], refs[2 * n_head : 3 * n_head]
    target_ref, relu_ref = refs[3 * n_head : 3 * n_head + 2]
    outs, (w_ref, grads, results) = refs[3 * n_head + 2 : -3], refs[-3:]
    rows = outs[0].shape[0]
    share, idx_width = parts[0].shape[1:]
    scale = 1.0 / idx_width**0.5
    lay_weights(parts, w_refs, w_ref)
    tile = w_ref.shape[1]
    start = lax.axis_index("head") * share
    slots, count = packed(ids, facts_ref)
    for i, (place, later, alive) in enumerate(slots):

        @pl.when(alive)
        def _(i=i, place=place, later=later):
            here = slice(i // 2 * rows, (i // 2 + 1) * rows)
            span = slice(i % 2 * share, (i % 2 + 1) * share)
            mass = masses[0][here, span]
            for other in masses[1:]:
                mass = mass + other[here, span]
            value = target_ref[here, span] - mass * (1.0 / HEADS)
            within = lax.broadcasted_iota(jnp.int32, (rows, share), 0)
            token = lax.broadcasted_iota(jnp.int32, (rows, share), 1) + start
            grad = jnp.where(within + later * rows <= token, value, 0.0)
            grads[at(place, rows), :] = jnp.concatenate([grad] * (tile // share), axis=1)

    def work(here):
        grad = grads[here, :]
        total = jnp.zeros((grad.shape[0], idx_width), jnp.float32)
        row = 0
        for part in parts:
            for run, piece in pieces(part, share, 8):
                weighted = []
                for k in range(row, row + run):
                    w = (grad * w_ref[k : k + 1, :]).astype(jnp.bfloat16)
                    r = relu_ref[here, k * tile : (k + 1) * tile]
                    weighted.append(jnp.where(r > 0, w, jnp.zeros_like(w)))
                row += run
                total = total + lax.dot_general(
                    jnp.concatenate(weighted, axis=1), piece, NN, preferred_element_type=jnp.float32
                )
        results[here, :] = total * scale

    in_pairs(count, len(ids), rows, work)
    for out, (place, _, alive) in zip(outs, slots):
        out[...] = jnp.where(alive, results[at(place, rows), :], 0.0)


def index_grad(known_facts, parts, weights, masses, target, relu, ids):
    n_head, (index_here, share, idx_width) = len(parts), parts[0].shape
    n, rows = len(ids), relu.shape[0] // len(ids)
    side = lanes_of(parts[0], share)
    return pl.pallas_call(
        functools.partial(grad_kernel, ids, n_head),
        in_specs=[SMEM] + [VMEM] * (3 * n_head + 2),
        out_specs=[VMEM] * n,
        out_shape=[jax.ShapeDtypeStruct((rows, idx_width), jnp.float32)] * n,
        scratch_shapes=[
            pltpu.VMEM((n_head * index_here // side, side * share), jnp.float32),
            pltpu.VMEM((n * rows, side * share), jnp.float32),
            pltpu.VMEM((n * rows, idx_width), jnp.float32),
        ],
        cost_estimate=cost(2 * n * rows * share * n_head * index_here * idx_width),
        compiler_params=pltpu.CompilerParams(vmem_limit_bytes=LIMIT),
        name="index_grad",
    )(known_facts, *parts, *weights, *masses, target, relu)


def body(
    q_main,
    latent_keys,
    lse_main,
    index_queries,
    index_weights,
    index_keys,
    lse_index,
    slab_order,
    block_live,
):
    n_seq = lax.axis_size("seq")
    n_head = lax.axis_size("head")
    latent = latent_keys.shape[1]
    devices = range(n_seq)

    def ring(distance):
        return [(i, (i + distance) % n_seq) for i in devices]

    def around(array, turn):
        return lax.ppermute(array, "head", [(i, (i + turn) % n_head) for i in range(n_head)])

    forward = [(i, (i + (HOPS - 1 if i % 2 else 1)) % n_seq) for i in devices]
    back = [(b, a) for a, b in forward]
    swap = [(i, i ^ 1) for i in devices]
    own = jnp.concatenate([latent_keys.T, index_keys], axis=0)
    own, shares = cut_shares(own, index_queries, n_head)
    arrived = [lax.ppermute(own, "seq", ring(2))]
    arrived.append(lax.ppermute(own, "seq", ring(4)))
    slots = [own, lax.ppermute(own, "seq", forward)]
    for m in range(1, HOPS // 2):
        if m > 2:
            arrived.append(lax.ppermute(arrived[m - 3], "seq", ring(4)))
        slots += [arrived[m - 1], lax.ppermute(arrived[m - 1], "seq", swap)]

    turns = range(n_head)
    weights = [around(index_weights.T, turn) if turn else index_weights.T for turn in turns]
    parts = [around(shares[turn], turn) if turn else shares[turn] for turn in turns]
    parts = [part.transpose(1, 0, 2) for part in parts]

    q, lse, lse_share = q_main.transpose(1, 2, 0), lse_main.T, lse_index[None, :]

    def blocks(ids):
        return [slots[i] for i in ids]

    runs = [(0,)] + [(2 * m, 2 * m + 1) for m in range(1, HOPS // 2 - 1)]
    runs[-1] += (1,)
    early = tuple(i for run in runs for i in run)
    late = (HOPS - 2, HOPS - 1)
    tables, own_mass = first_mass(slab_order, block_live, q, lse, own)
    known = [own_mass]
    for run in runs[1:-1]:
        known += head_mass(tables, q, lse, run, blocks(run))
    group = head_mass(tables, q, lse, runs[-1], blocks(runs[-1]), known, n_head)
    masses = [list(group)]
    masses.append(list(head_mass(tables, q, lse, late, blocks(late), (), n_head)))
    grads = {}
    for ids, mass in zip((early, late), masses):
        for turn in range(1, n_head):
            mass[turn] = around(mass[turn], turn)
        target, relu = index_logits(tables, parts, weights, lse_share, ids, blocks(ids), latent)
        found = index_grad(tables, parts, weights, mass, target, relu, ids)
        grads.update(zip(ids, found))

    total = grads[0] + lax.ppermute(grads[1], "seq", back)
    for m in range(1, HOPS // 2):
        both = grads[2 * m] + lax.ppermute(grads[2 * m + 1], "seq", swap)
        if m < HOPS // 2 - 1:
            total = total + lax.ppermute(both, "seq", ring(-2 * m))
    if n_head != 2:
        return lax.psum(total + lax.ppermute(both, "seq", ring(-2 * m)), "head")
    last = []
    for turn in range(2):
        route = [
            (2 * i + x, 2 * ((i - 2 * m) % n_seq) + (x + turn) % 2) for i in devices for x in range(2)
        ]
        last.append(lax.ppermute(both.astype(jnp.bfloat16), ("seq", "head"), route))
    total = total + around(total, 1)
    return total + (last[0].astype(jnp.float32) + last[1].astype(jnp.float32))


def solution(mesh):
    placed = (
        P("seq", "head", None),
        P("seq", None),
        P("seq", "head"),
        P("seq", "head", None),
        P("seq", "head"),
        P("seq", None),
        P("seq"),
        P(),
        P(),
    )
    return jax.shard_map(
        body, mesh=mesh, in_specs=placed, out_specs=P("seq", None), check_vma=False
    )
```

```python
import functools
import math

import jax
import jax.numpy as jnp
from jax import lax
from jax.experimental import pallas as pl
from jax.experimental.pallas import tpu as pltpu
from jax.sharding import PartitionSpec as P


HEADS = 128
HOPS = 8
LOG2E = math.log2(math.e)
MAIN_SCALE = 1.0 / 192.0**0.5
LIMIT = 20 * 2**20
CUT_COST = 10**10
NT = (((1,), (1,)), ((), ()))
NN = (((1,), (0,)), ((), ()))
VMEM = pl.BlockSpec(memory_space=pltpu.VMEM)
SMEM = pl.BlockSpec(memory_space=pltpu.SMEM)
HBM = pl.BlockSpec(memory_space=pltpu.HBM)


def cut_kernel(block_ref, queries_ref, block_out, *rest):
    del block_ref, block_out
    shares, sems = rest[:-1], rest[-1]
    n, share = len(shares), shares[0].shape[0]
    copies = []
    for turn, out in enumerate(shares):
        start = lax.rem(lax.axis_index("head") + turn, n) * share
        part = queries_ref.at[pl.ds(start, share)]
        copies.append(pltpu.make_async_copy(part, out, sems.at[turn]))
    for copy in copies:
        copy.start()
    for copy in copies:
        copy.wait()


def cut_shares(block, index_queries, n_head):
    tokens, index_here, idx_width = index_queries.shape
    share = jax.ShapeDtypeStruct((tokens // n_head, index_here, idx_width), index_queries.dtype)
    block, *shares = pl.pallas_call(
        cut_kernel,
        in_specs=[VMEM, HBM],
        out_specs=[VMEM] * (1 + n_head),
        out_shape=[jax.ShapeDtypeStruct(block.shape, block.dtype)] + [share] * n_head,
        input_output_aliases={0: 0},
        scratch_shapes=[pltpu.SemaphoreType.DMA((n_head,))],
        cost_estimate=cost(CUT_COST),
        compiler_params=pltpu.CompilerParams(vmem_limit_bytes=LIMIT),
        name="cut_shares",
    )(block, index_queries)
    return block, shares


def facts(slot, order_ref, live_ref):
    n = lax.axis_size("seq")
    me = lax.axis_index("seq")
    crossed = (slot % 2 == 1) & (me % 2 == 0)
    hop = jnp.where(crossed, jnp.where(slot == 1, HOPS - 1, slot - 2), slot)
    own = order_ref[me]
    slab = order_ref[lax.rem(me - hop + n, n)]
    return slab - own, (slab <= own) & (live_ref[own, slab] == 1)


def packed(ids, facts_ref):
    count, slots = jnp.int32(0), []
    for i in ids:
        alive = facts_ref[2 * i + 1]
        slots.append((count, facts_ref[2 * i], alive == 1))
        count = count + alive
    return slots, count


def side_by_side(values):
    if len(values) % 2:
        values = values + [jnp.zeros_like(values[0])]
    pairs = [jnp.concatenate(values[i : i + 2], axis=1) for i in range(0, len(values), 2)]
    return jnp.concatenate(pairs, axis=0)


def side_by_side_shape(n, rows, share):
    return jax.ShapeDtypeStruct(((n + 1) // 2 * rows, 2 * share), jnp.float32)


def at(place, rows, blocks=1):
    return pl.ds(pl.multiple_of(place * rows, rows), blocks * rows)


def in_pairs(count, most, rows, work):
    def two(i, carry):
        work(at(2 * i, rows, 2))
        return carry

    if most == 2:
        pl.when(count == 2)(lambda: work(pl.ds(0, 2 * rows)))
    elif most > 2:
        lax.fori_loop(0, count // 2, two, 0)

    @pl.when(count % 2 == 1)
    def _():
        work(at(count - 1, rows))


def cost(flops):
    return pl.CostEstimate(flops=flops, transcendentals=0, bytes_accessed=flops // 256)


def mass_of(keys, q_ref, lse_ref):
    heads, _, tokens = q_ref.shape
    total = None
    for h in range(0, heads, 2):
        pair = jnp.concatenate([q_ref[h], q_ref[h + 1]], axis=1)
        s = lax.dot_general(keys, pair, NN, preferred_element_type=jnp.float32)
        s = s * (MAIN_SCALE * LOG2E)
        for n in range(2):
            lse = lse_ref[h + n : h + n + 1, :] * LOG2E
            p = jnp.exp2(s[:, n * tokens : (n + 1) * tokens] - lse)
            total = p if total is None else total + p
    return total


def score_kernel(ids, n_outs, pack, facts_ref, q_ref, lse_ref, *refs):
    blocks, known = refs[: len(ids)], refs[len(ids) : -n_outs - 2]
    outs, (keys, mass) = refs[-n_outs - 2 : -2], refs[-2:]
    latent, tokens = q_ref.shape[1:]
    rows = blocks[0].shape[1]
    slots, count = packed(ids, facts_ref)
    for block, (place, _, alive) in zip(blocks, slots):

        @pl.when(alive)
        def _(block=block, place=place):
            keys[at(place, rows), :] = block[:latent, :].T

    def work(here):
        mass[here, :] = mass_of(keys[here, :], q_ref, lse_ref)

    in_pairs(count, len(blocks), rows, work)
    values = [jnp.where(alive, mass[at(place, rows), :], 0.0) for place, _, alive in slots]
    if not pack:
        for out, value in zip(outs, values):
            out[...] = value
        return
    values = [ref[...] for ref in known] + values
    share = tokens // n_outs
    if n_outs > 1:
        turn = tokens - lax.axis_index("head") * share
        values = [pltpu.roll(value, turn, 1) for value in values]
    for n, out in enumerate(outs):
        out[...] = side_by_side([value[:, n * share : (n + 1) * share] for value in values])


def head_mass(known_facts, q, lse, ids, blocks, known=(), n_head=0):
    heads, latent, tokens = q.shape
    n, rows = len(ids), blocks[0].shape[1]
    shapes = [jax.ShapeDtypeStruct((rows, tokens), jnp.float32)] * n
    if n_head:
        shapes = [side_by_side_shape(n + len(known), rows, tokens // n_head)] * n_head
    return pl.pallas_call(
        functools.partial(score_kernel, ids, len(shapes), n_head > 0),
        in_specs=[SMEM] + [VMEM] * (2 + n + len(known)),
        out_specs=[VMEM] * len(shapes),
        out_shape=shapes,
        scratch_shapes=[
            pltpu.VMEM((n * rows, latent), jnp.bfloat16),
            pltpu.VMEM((n * rows, tokens), jnp.float32),
        ],
        cost_estimate=cost(2 * tokens * heads * latent * n * rows),
        compiler_params=pltpu.CompilerParams(vmem_limit_bytes=LIMIT),
        name="score_mass",
    )(known_facts, q, lse, *blocks, *known)


def first_kernel(order_ref, live_ref, q_ref, lse_ref, block_ref, facts_ref, mass_ref):
    own_alive = facts(0, order_ref, live_ref)[1]
    mass = mass_of(block_ref[: q_ref.shape[1], :].T, q_ref, lse_ref)
    mass_ref[...] = jnp.where(own_alive, mass, 0.0)
    for i in range(HOPS):
        later, alive = facts(i, order_ref, live_ref)
        facts_ref[2 * i] = later
        facts_ref[2 * i + 1] = alive.astype(jnp.int32)


def first_mass(order, live, q, lse, block):
    heads, latent, tokens = q.shape
    rows = block.shape[1]
    return pl.pallas_call(
        first_kernel,
        in_specs=[SMEM, SMEM] + [VMEM] * 3,
        out_specs=[SMEM, VMEM],
        out_shape=[
            jax.ShapeDtypeStruct((2 * HOPS,), jnp.int32),
            jax.ShapeDtypeStruct((rows, tokens), jnp.float32),
        ],
        cost_estimate=cost(2 * tokens * heads * latent * rows),
        compiler_params=pltpu.CompilerParams(vmem_limit_bytes=LIMIT),
        name="first_mass",
    )(order, live, q, lse, block)


def lanes_of(part, share):
    return max(1, min(part.shape[0], 128 // share))


def pieces(part, share, width):
    side = lanes_of(part, share)
    step = part.shape[0] // side
    run = max(1, min(step, width))
    for first in range(0, step, run):
        heads = [part[k + n * step] for k in range(first, first + run) for n in range(side)]
        yield run, jnp.concatenate(heads, axis=0)


def lay_weights(parts, w_refs, w_lanes):
    row = 0
    for part, w_ref in zip(parts, w_refs):
        index_here, tokens = w_ref.shape
        share = part.shape[1]
        w = w_ref[...]
        if share < tokens:
            w = pltpu.roll(w, tokens - lax.axis_index("head") * share, 1)
        side = lanes_of(part, share)
        step = index_here // side
        tile = [w[n * step : (n + 1) * step, :share] for n in range(side)]
        w_lanes[row : row + step, :] = jnp.concatenate(tile, axis=1)
        row += step


def logit_kernel(latent, ids, n_head, facts_ref, *refs):
    parts, w_refs, lse_ref = refs[:n_head], refs[n_head : 2 * n_head], refs[2 * n_head]
    blocks, (out_ref, relu_ref, w_ref, keys, values) = refs[2 * n_head + 1 : -5], refs[-5:]
    rows, idx_width = blocks[0].shape[1], keys.shape[1]
    share = parts[0].shape[1]
    scale = 1.0 / idx_width**0.5
    lay_weights(parts, w_refs, w_ref)
    tile = w_ref.shape[1]
    lse = lse_ref[...]
    if share < lse.shape[1]:
        lse = pltpu.roll(lse, lse.shape[1] - lax.axis_index("head") * share, 1)[:, :share]
    slots, count = packed(ids, facts_ref)
    for block, (place, _, alive) in zip(blocks, slots):

        @pl.when(alive)
        def _(block=block, place=place):
            keys[at(place, rows), :] = block[latent:, :]

    def work(here):
        held = keys[here, :]
        acc = jnp.zeros((held.shape[0], tile), jnp.float32)
        row = 0
        for part in parts:
            for run, piece in pieces(part, share, 8):
                r = lax.dot_general(held, piece, NT, preferred_element_type=jnp.float32)
                relu_ref[here, row * tile : (row + run) * tile] = r.astype(jnp.bfloat16)
                for k in range(run):
                    relu = jnp.maximum(r[:, k * tile : (k + 1) * tile], 0.0)
                    acc = acc + relu * w_ref[row + k : row + k + 1, :]
                row += run
        logits = acc[:, :share]
        for first in range(share, tile, share):
            logits = logits + acc[:, first : first + share]
        values[here, :] = jnp.exp(logits * scale - lse)

    in_pairs(count, len(blocks), rows, work)
    out_ref[...] = side_by_side([jnp.where(s[2], values[at(s[0], rows), :], 0.0) for s in slots])


def index_logits(known_facts, parts, weights, lse, ids, blocks, latent):
    n_head, (index_here, share, idx_width) = len(parts), parts[0].shape
    rows = blocks[0].shape[1]
    side = lanes_of(parts[0], share)
    return pl.pallas_call(
        functools.partial(logit_kernel, latent, ids, n_head),
        in_specs=[SMEM] + [VMEM] * (2 * n_head + 1 + len(blocks)),
        out_specs=[VMEM, VMEM],
        out_shape=[
            side_by_side_shape(len(blocks), rows, share),
            jax.ShapeDtypeStruct((len(blocks) * rows, n_head * index_here * share), jnp.bfloat16),
        ],
        scratch_shapes=[
            pltpu.VMEM((n_head * index_here // side, side * share), jnp.float32),
            pltpu.VMEM((len(blocks) * rows, idx_width), jnp.bfloat16),
            pltpu.VMEM((len(blocks) * rows, share), jnp.float32),
        ],
        cost_estimate=cost(2 * len(blocks) * rows * share * n_head * index_here * idx_width),
        compiler_params=pltpu.CompilerParams(vmem_limit_bytes=LIMIT),
        name="index_logits",
    )(known_facts, *parts, *weights, lse, *blocks)


def grad_kernel(ids, n_head, facts_ref, *refs):
    parts, w_refs, masses = refs[:n_head], refs[n_head : 2 * n_head], refs[2 * n_head : 3 * n_head]
    target_ref, relu_ref = refs[3 * n_head : 3 * n_head + 2]
    outs, (w_ref, grads, results) = refs[3 * n_head + 2 : -3], refs[-3:]
    rows = outs[0].shape[0]
    share, idx_width = parts[0].shape[1:]
    scale = 1.0 / idx_width**0.5
    lay_weights(parts, w_refs, w_ref)
    tile = w_ref.shape[1]
    start = lax.axis_index("head") * share
    slots, count = packed(ids, facts_ref)
    for i, (place, later, alive) in enumerate(slots):

        @pl.when(alive)
        def _(i=i, place=place, later=later):
            here = slice(i // 2 * rows, (i // 2 + 1) * rows)
            span = slice(i % 2 * share, (i % 2 + 1) * share)
            mass = masses[0][here, span]
            for other in masses[1:]:
                mass = mass + other[here, span]
            value = target_ref[here, span] - mass * (1.0 / HEADS)
            within = lax.broadcasted_iota(jnp.int32, (rows, share), 0)
            token = lax.broadcasted_iota(jnp.int32, (rows, share), 1) + start
            grad = jnp.where(within + later * rows <= token, value, 0.0)
            grads[at(place, rows), :] = jnp.concatenate([grad] * (tile // share), axis=1)

    def work(here):
        grad = grads[here, :]
        total = jnp.zeros((grad.shape[0], idx_width), jnp.float32)
        row = 0
        for part in parts:
            for run, piece in pieces(part, share, 8):
                weighted = []
                for k in range(row, row + run):
                    w = (grad * w_ref[k : k + 1, :]).astype(jnp.bfloat16)
                    r = relu_ref[here, k * tile : (k + 1) * tile]
                    weighted.append(jnp.where(r > 0, w, jnp.zeros_like(w)))
                row += run
                total = total + lax.dot_general(
                    jnp.concatenate(weighted, axis=1), piece, NN, preferred_element_type=jnp.float32
                )
        results[here, :] = total * scale

    in_pairs(count, len(ids), rows, work)
    for out, (place, _, alive) in zip(outs, slots):
        out[...] = jnp.where(alive, results[at(place, rows), :], 0.0)


def index_grad(known_facts, parts, weights, masses, target, relu, ids):
    n_head, (index_here, share, idx_width) = len(parts), parts[0].shape
    n, rows = len(ids), relu.shape[0] // len(ids)
    side = lanes_of(parts[0], share)
    return pl.pallas_call(
        functools.partial(grad_kernel, ids, n_head),
        in_specs=[SMEM] + [VMEM] * (3 * n_head + 2),
        out_specs=[VMEM] * n,
        out_shape=[jax.ShapeDtypeStruct((rows, idx_width), jnp.float32)] * n,
        scratch_shapes=[
            pltpu.VMEM((n_head * index_here // side, side * share), jnp.float32),
            pltpu.VMEM((n * rows, side * share), jnp.float32),
            pltpu.VMEM((n * rows, idx_width), jnp.float32),
        ],
        cost_estimate=cost(2 * n * rows * share * n_head * index_here * idx_width),
        compiler_params=pltpu.CompilerParams(vmem_limit_bytes=LIMIT),
        name="index_grad",
    )(known_facts, *parts, *weights, *masses, target, relu)


def body(
    q_main,
    latent_keys,
    lse_main,
    index_queries,
    index_weights,
    index_keys,
    lse_index,
    slab_order,
    block_live,
):
    n_seq = lax.axis_size("seq")
    n_head = lax.axis_size("head")
    latent = latent_keys.shape[1]
    devices = range(n_seq)

    def ring(distance):
        return [(i, (i + distance) % n_seq) for i in devices]

    def around(array, turn):
        return lax.ppermute(array, "head", [(i, (i + turn) % n_head) for i in range(n_head)])

    forward = [(i, (i + (HOPS - 1 if i % 2 else 1)) % n_seq) for i in devices]
    back = [(b, a) for a, b in forward]
    swap = [(i, i ^ 1) for i in devices]
    own = jnp.concatenate([latent_keys.T, index_keys], axis=0)
    own, shares = cut_shares(own, index_queries, n_head)
    arrived = [lax.ppermute(own, "seq", ring(2))]
    arrived.append(lax.ppermute(own, "seq", ring(4)))
    slots = [own, lax.ppermute(own, "seq", forward)]
    for m in range(1, HOPS // 2):
        if m > 2:
            arrived.append(lax.ppermute(arrived[m - 3], "seq", ring(4)))
        slots += [arrived[m - 1], lax.ppermute(arrived[m - 1], "seq", swap)]

    turns = range(n_head)
    weights = [around(index_weights.T, turn) if turn else index_weights.T for turn in turns]
    parts = [around(shares[turn], turn) if turn else shares[turn] for turn in turns]
    parts = [part.transpose(1, 0, 2) for part in parts]

    q, lse, lse_share = q_main.transpose(1, 2, 0), lse_main.T, lse_index[None, :]

    def blocks(ids):
        return [slots[i] for i in ids]

    runs = [(0,)] + [(2 * m, 2 * m + 1) for m in range(1, HOPS // 2 - 1)]
    runs[-1] += (1,)
    early = tuple(i for run in runs for i in run)
    late = (HOPS - 2, HOPS - 1)
    tables, own_mass = first_mass(slab_order, block_live, q, lse, own)
    known = [own_mass]
    for run in runs[1:-1]:
        known += head_mass(tables, q, lse, run, blocks(run))
    group = head_mass(tables, q, lse, runs[-1], blocks(runs[-1]), known, n_head)
    masses = [list(group)]
    masses.append(list(head_mass(tables, q, lse, late, blocks(late), (), n_head)))
    grads = {}
    for ids, mass in zip((early, late), masses):
        for turn in range(1, n_head):
            mass[turn] = around(mass[turn], turn)
        target, relu = index_logits(tables, parts, weights, lse_share, ids, blocks(ids), latent)
        found = index_grad(tables, parts, weights, mass, target, relu, ids)
        grads.update(zip(ids, found))

    total = grads[0] + lax.ppermute(grads[1], "seq", back)
    for m in range(1, HOPS // 2):
        both = grads[2 * m] + lax.ppermute(grads[2 * m + 1], "seq", swap)
        if m < HOPS // 2 - 1:
            total = total + lax.ppermute(both, "seq", ring(-2 * m))
    if n_head != 2:
        return lax.psum(total + lax.ppermute(both, "seq", ring(-2 * m)), "head")
    last = []
    for turn in range(2):
        route = [
            (2 * i + x, 2 * ((i - 2 * m) % n_seq) + (x + turn) % 2) for i in devices for x in range(2)
        ]
        last.append(lax.ppermute(both.astype(jnp.bfloat16), ("seq", "head"), route))
    total = total + around(total, 1)
    return total + (last[0].astype(jnp.float32) + last[1].astype(jnp.float32))


def solution(mesh):
    placed = (
        P("seq", "head", None),
        P("seq", None),
        P("seq", "head"),
        P("seq", "head", None),
        P("seq", "head"),
        P("seq", None),
        P("seq"),
        P(),
        P(),
    )
    return jax.shard_map(
        body, mesh=mesh, in_specs=placed, out_specs=P("seq", None), check_vma=False
    )
```
